512 devices in a mesh: section: 16 (over z), dp: 32 (over y, x, core).
Axes of the slice: x: 4, y: 4, z: 16, core: 2. Of those that a mesh axis runs over, the one named last changes fastest.
Arguments:
- acts: bfloat16 [16, 4, 32, 12, 16, 512], P('section', None, 'dp'), may hold values from -6 to 6
- out_grad: bfloat16 [4, 32, 12, 16, 512], P(None, 'dp'), may hold values from -6 to 6
- depth_kernel: bfloat16 [16, 3, 3, 512], P('section'), may hold values from -2 to 2
- point_weight: bfloat16 [16, 512, 512], P('section'), may hold values from -0.25 to 0.25
- bn_gain: float32 [16, 512], P('section'), may hold values from 0.15 to 0.45
Outputs:
- act_grad: bfloat16 [16, 4, 32, 12, 16, 512], P('section', None, 'dp')
- point_grad: float32 [16, 512, 512], P('section')
- kernel_grad: float32 [16, 3, 3, 512], P('section')
- gain_grad: float32 [16, 512], P('section')
- bias_grad: float32 [16, 512], P('section')
The draws below stay inside these ranges and needn't reach their ends.
All inputs are finite; a program needn't handle non-finite values.
Results may differ from the reference program's by a relative error of at most 0.025.
Values may be sent and summed in bfloat16 or wider, within the bound.
A program may use at most 64 MiB of HBM per device.

```python
import jax
import jax.numpy as jnp
from jax import lax

CHANNELS = 512
HEIGHT = 12
WIDTH = 16
MICRO = 4
SECTIONS = 16
IMAGES = 32


def steps_of(key, dims, cuts, low, top_value):
    level = 1.0
    for axis_at, parts in cuts:
        heights = jax.random.uniform(jax.random.fold_in(jax.random.fold_in(key, 6), axis_at), (parts,), jnp.float32, low / len(cuts), top_value / len(cuts))
        level = level * jnp.repeat(jnp.exp(heights), dims[axis_at] // parts).reshape((-1,) + (1,) * (len(dims) - 1 - axis_at))
    return level


def centred(rng, shape, scale, limit, pieces=(), kind=jnp.bfloat16):
    result = scale * jax.random.normal(rng, shape, jnp.float32)
    if pieces:
        result = result * steps_of(rng, shape, pieces, -0.22, 0.18)
    return jnp.clip(result, -limit, limit).astype(kind)


def setup_inputs(seed: int = 0) -> dict:
    key_list = jax.random.split(jax.random.key(seed), 6)
    return {
        "acts": centred(key_list[0], (SECTIONS, MICRO, IMAGES, HEIGHT, WIDTH, CHANNELS), 1.0, 6.0, ((0, 16), (2, 32))),
        "out_grad": centred(key_list[1], (MICRO, IMAGES, HEIGHT, WIDTH, CHANNELS), 1.0, 6.0, ((1, 32),)),
        "depth_kernel": centred(key_list[2], (SECTIONS, 3, 3, CHANNELS), 9 ** -0.5, 2.0, ((0, 16),)),
        "point_weight": centred(key_list[3], (SECTIONS, CHANNELS, CHANNELS), CHANNELS ** -0.5, 0.25, ((0, 16),)),
        "bn_gain": jnp.clip(0.15 + 0.29999998 * jax.random.uniform(key_list[4], (SECTIONS, CHANNELS), jnp.float32) ** steps_of(key_list[4], (SECTIONS, CHANNELS), ((0, 16),), -0.2, 0.2), 0.15, 0.45),
    }


epsilon = 1e-05

def depthwise(active, kernel):
    padded = jnp.pad(active, ((0, 0), (1, 1), (1, 1), (0, 0)))
    height, width = (active.shape[1], active.shape[2])
    summed = jnp.zeros(active.shape, jnp.float32)
    for row_off in range(3):
        for col_off in range(3):
            summed = summed + kernel[row_off, col_off] * padded[:, row_off:row_off + height, col_off:col_off + width]
    return summed

def depthwise_back(grad, kernel):
    padded = jnp.pad(grad, ((0, 0), (1, 1), (1, 1), (0, 0)))
    height, width = (grad.shape[1], grad.shape[2])
    summed = jnp.zeros(grad.shape, jnp.float32)
    for row_off in range(3):
        for col_off in range(3):
            summed = summed + kernel[row_off, col_off] * padded[:, 2 - row_off:2 - row_off + height, 2 - col_off:2 - col_off + width]
    return summed

def kernel_terms(active, grad):
    padded = jnp.pad(active, ((0, 0), (1, 1), (1, 1), (0, 0)))
    height, width = (active.shape[1], active.shape[2])
    table = []
    for row_off in range(3):
        line = []
        for col_off in range(3):
            line.append(lax.optimization_barrier(jnp.sum(padded[:, row_off:row_off + height, col_off:col_off + width] * grad, axis=(0, 1, 2))))
        table.append(jnp.stack(line))
    return jnp.stack(table)

def reference(acts, out_grad, depth_kernel, point_weight, bn_gain):
    count = IMAGES * HEIGHT * WIDTH
    shape = (IMAGES, HEIGHT, WIDTH, CHANNELS)
    below = None
    grads_all, points_all, kernels_all, gains_all, biases_all = ([], [], [], [], [])
    for section in reversed(range(SECTIONS)):
        kernel = depth_kernel[section].astype(jnp.float32)
        weight = point_weight[section]
        gain = bn_gain[section]
        point_acc = jnp.zeros((CHANNELS, CHANNELS), jnp.float32)
        kernel_acc = jnp.zeros((3, 3, CHANNELS), jnp.float32)
        gain_acc = jnp.zeros((CHANNELS,), jnp.float32)
        bias_acc = jnp.zeros((CHANNELS,), jnp.float32)
        results = []
        for micro in range(MICRO):
            inputs = acts[section, micro]
            active = jnp.maximum(inputs.astype(jnp.float32), 0.0)
            depth_out = depthwise(active, kernel).astype(jnp.bfloat16).reshape(-1, CHANNELS)
            pre_norm = jnp.dot(depth_out, weight, preferred_element_type=jnp.float32)
            center = lax.optimization_barrier(jnp.sum(pre_norm, axis=0)) / count
            square = lax.optimization_barrier(jnp.sum(pre_norm * pre_norm, axis=0)) / count
            inv_std = lax.rsqrt(square - center * center + epsilon)
            normed = (pre_norm - center) * inv_std
            if section == SECTIONS - 1:
                upstream = out_grad[micro]
            else:
                upstream = below[micro]
            upstream = upstream.astype(jnp.float32).reshape(-1, CHANNELS)
            sum_grad = lax.optimization_barrier(jnp.sum(upstream, axis=0))
            sum_cross = lax.optimization_barrier(jnp.sum(upstream * normed, axis=0))
            gain_acc = gain_acc + sum_cross
            bias_acc = bias_acc + sum_grad
            pre_grad = (gain * inv_std * (upstream - sum_grad / count - normed * sum_cross / count)).astype(jnp.bfloat16)
            point_acc = point_acc + jnp.dot(depth_out.T, pre_grad, preferred_element_type=jnp.float32)
            depth_grad = jnp.dot(pre_grad, weight.T, preferred_element_type=jnp.float32).reshape(shape)
            kernel_acc = kernel_acc + kernel_terms(active, depth_grad)
            back = depthwise_back(depth_grad, kernel)
            input_grad = upstream.reshape(shape) + jnp.where(inputs > 0, back, 0.0)
            results.append(input_grad.astype(jnp.bfloat16))
        below = results
        grads_all.append(jnp.stack(results))
        points_all.append(point_acc)
        kernels_all.append(kernel_acc)
        gains_all.append(gain_acc)
        biases_all.append(bias_acc)
    act_grad = jnp.stack(grads_all[::-1])
    point_grad = jnp.stack(points_all[::-1])
    kernel_grad = jnp.stack(kernels_all[::-1])
    gain_grad = jnp.stack(gains_all[::-1])
    bias_grad = jnp.stack(biases_all[::-1])
    return (act_grad, point_grad, kernel_grad, gain_grad, bias_grad)
```

```python
import functools

import jax
import jax.numpy as jnp
from jax import lax
from jax.experimental import pallas as pl
from jax.experimental.pallas import tpu as pltpu
from jax.sharding import PartitionSpec as P

MESH = pl.DeviceIdType.MESH
epsilon = 1e-05
LANES = 128


def columns_of(x, width):
    rows = x.shape[0]
    at = lax.broadcasted_iota(jnp.int32, x.shape, 0) % width
    before = jnp.where(at == 0, 0.0, pltpu.roll(x, 1, 0))
    after = jnp.where(at == width - 1, 0.0, pltpu.roll(x, rows - 1, 0))
    return before, x, after


def down(x, width):
    return jnp.concatenate([jnp.zeros((width, x.shape[1]), x.dtype), x[:-width]], axis=0)


def up(x, width):
    return jnp.concatenate([x[width:], jnp.zeros((width, x.shape[1]), x.dtype)], axis=0)


def kernel(
    sections, replicas, micros, height, width, channels,
    acts, out_grad, kern, weight, gain,
    out, point, kgrad, ggrad, bgrad,
    x_v, w_v, kf, depth, normed, nsend, nrecv, ubuf, usend, pgs, dgs,
    sbuf, smsg, omsg, tbuf, tmsg, stat, gacc,
    pacc, rs_src, rs_buf, ag_src, ag_buf, kacc, krs_buf, kag_src, kag_buf,
    in_sem, og_sem, out_sem,
    t_send, t_recv, n_send, n_recv, u_send, u_recv, s_send, s_recv, o_send,
    rs_send, rs_recv, ag_send, ag_recv, ks_send, ks_recv, kg_send, kg_recv,
):
    f32, bf16 = jnp.float32, jnp.bfloat16
    sec = lax.axis_index("section")
    me = lax.axis_index("dp")
    rows = height * width
    chunks = channels // LANES
    count = replicas * rows
    last = sections - 1
    below = (sec + sections - 1) % sections
    above = (sec + 1) % sections

    def lanes(c):
        return slice(c * LANES, (c + 1) * LANES)

    for m in range(micros):
        pltpu.make_async_copy(acts.at[0, m, 0], x_v.at[m], in_sem.at[m]).start()
        if m == 0:
            pltpu.make_async_copy(weight.at[0], w_v, in_sem.at[micros]).start()

    @pl.when(sec == last)
    def _():
        for m in range(micros):
            pltpu.make_async_copy(out_grad.at[m, 0], ubuf.at[m], og_sem.at[m]).start()

    barrier = pltpu.get_barrier_semaphore()

    def greet(k, _):
        peer = (me + k) % replicas
        pl.semaphore_signal(barrier, inc=1, device_id={"section": below, "dp": peer}, device_id_type=MESH)
        pl.semaphore_signal(barrier, inc=1, device_id={"section": above, "dp": peer}, device_id_type=MESH)

        @pl.when(k > 0)
        def _():
            pl.semaphore_signal(barrier, inc=1, device_id={"section": sec, "dp": peer}, device_id_type=MESH)

        return 0

    lax.fori_loop(0, replicas, greet, 0)

    for i in range(3):
        for j in range(3):
            kf[3 * i + j] = jnp.reshape(kern[0, i, j].astype(f32), (1, channels))
    kacc[...] = jnp.zeros(kacc.shape, f32)
    gacc[...] = jnp.zeros(gacc.shape, f32)
    pacc[...] = jnp.zeros(pacc.shape, f32)

    def tap(i, j, c):
        return kf[3 * i + j, :, lanes(c)]

    def to_plane(section, src, dst, send, recv, first):
        def one(k, _):
            peer = (me + k) % replicas
            pltpu.make_async_remote_copy(
                src_ref=src(peer), dst_ref=dst, send_sem=send, recv_sem=recv,
                device_id={"section": section, "dp": peer}, device_id_type=MESH,
            ).start()
            return 0

        lax.fori_loop(first, replicas, one, 0)

    def wait_bytes(ref, sem):
        pltpu.make_async_copy(ref, ref, sem).wait()

    def row_sum(x):
        return jnp.sum(x, axis=0, keepdims=True)

    def forward(m, _):
        pltpu.make_async_copy(acts.at[0, m, 0], x_v.at[m], in_sem.at[m]).wait()
        for c in range(chunks):
            x = x_v[m, :, :, lanes(c)].astype(f32).reshape(rows, LANES)
            parts = columns_of(jnp.maximum(x, 0.0), width)
            line = [sum(tap(i, j, c) * parts[j] for j in range(3)) for i in range(3)]
            depth[m, :, lanes(c)] = (down(line[0], width) + line[1] + up(line[2], width)).astype(bf16)

        @pl.when(m == 0)
        def _():
            pltpu.make_async_copy(weight.at[0], w_v, in_sem.at[micros]).wait()

        normed[m] = jnp.dot(depth[m], w_v[...], preferred_element_type=f32)
        for c in range(chunks):
            pre = normed[m, :, lanes(c)]
            tmsg[m, c : c + 1, :] = row_sum(pre)
            tmsg[m, chunks + c : chunks + c + 1, :] = row_sum(pre * pre)

        @pl.when(m == 0)
        def _():
            pl.semaphore_wait(barrier, 3 * replicas - 1)

        tbuf[m, me] = tmsg[m]
        to_plane(sec, lambda _: tmsg.at[m], tbuf.at[m, me], t_send, t_recv.at[m], 1)

        @pl.when(sec == last)
        def _():
            pltpu.make_async_copy(out_grad.at[m, 0], ubuf.at[m], og_sem.at[m]).wait()
            for c in range(chunks):
                u = ubuf[m, :, :, lanes(c)].astype(f32).reshape(rows, LANES)
                omsg[m, c : c + 1, :] = row_sum(u)
                omsg[m, chunks + c : chunks + c + 1, :] = row_sum(u * normed[m, :, lanes(c)])
            sbuf[m, me] = omsg[m]
            to_plane(sec, lambda _: omsg.at[m], sbuf.at[m, me], o_send, s_recv.at[m], 1)

        return 0

    lax.fori_loop(0, micros, forward, 0)

    def normalise(m, _):
        wait_bytes(tbuf.at[m, pl.ds(0, replicas - 1)], t_recv.at[m])
        total = jnp.sum(tbuf[m], axis=0) / count
        center = total[:chunks]
        inv_std = lax.rsqrt(total[chunks:] - center * center + epsilon)
        stat[m, 0:chunks, :] = center
        stat[m, chunks:, :] = inv_std
        for c in range(chunks):
            value = (normed[m, :, lanes(c)] - center[c : c + 1]) * inv_std[c : c + 1]
            normed[m, :, lanes(c)] = value
            nsend[m, :, lanes(c)] = value.astype(bf16)

        @pl.when(sec < last)
        def _():
            pltpu.make_async_remote_copy(
                src_ref=nsend.at[m], dst_ref=nrecv.at[m], send_sem=n_send, recv_sem=n_recv.at[m],
                device_id={"section": above, "dp": me}, device_id_type=MESH,
            ).start()

        return 0

    lax.fori_loop(0, micros, normalise, 0)

    def backward(m, _):
        @pl.when(sec == last)
        def _():
            wait_bytes(sbuf.at[m, pl.ds(0, replicas - 1)], s_recv.at[m])

        @pl.when(sec < last)
        def _():
            wait_bytes(sbuf.at[m], s_recv.at[m])
            wait_bytes(ubuf.at[m], u_recv.at[m])

        total = jnp.sum(sbuf[m], axis=0)
        center, inv_std = stat[m, 0:chunks, :], stat[m, chunks:, :]
        sum_grad, cross = total[:chunks], total[chunks:]
        cross = jnp.where(sec == last, inv_std * (cross - center * sum_grad), cross)
        gacc[0:chunks, :] += sum_grad
        gacc[chunks:, :] += cross
        for c in range(chunks):
            scale = gain[0:1, lanes(c)] * inv_std[c : c + 1]
            shift = scale * sum_grad[c : c + 1] / count
            slope = scale * cross[c : c + 1] / count
            u = ubuf[m, :, :, lanes(c)].astype(f32).reshape(rows, LANES)
            pgs[:, lanes(c)] = (scale * u - shift - slope * normed[m, :, lanes(c)]).astype(bf16)
        dgs[...] = lax.dot_general(pgs[...], w_v[...], (((1,), (1,)), ((), ())), preferred_element_type=f32)

        @pl.when(sec > 0)
        def _():
            wait_bytes(nrecv.at[m], n_recv.at[m])

        for c in range(chunks):
            after, same, before = columns_of(dgs[:, lanes(c)], width)[::-1]
            parts = (after, same, before)
            line = [sum(tap(i, j, c) * parts[j] for j in range(3)) for i in range(3)]
            back = up(line[0], width) + line[1] + down(line[2], width)
            u = ubuf[m, :, :, lanes(c)].astype(f32).reshape(rows, LANES)
            x = x_v[m, :, :, lanes(c)].astype(f32).reshape(rows, LANES)
            result = (u + jnp.where(x > 0, back, 0.0)).astype(bf16)
            usend[m, :, :, lanes(c)] = result.reshape(height, width, LANES)

            @pl.when(sec > 0)
            def _():
                pltpu.make_async_remote_copy(
                    src_ref=usend.at[m, :, :, pl.ds(c * LANES, LANES)],
                    dst_ref=ubuf.at[m, :, :, pl.ds(c * LANES, LANES)],
                    send_sem=u_send, recv_sem=u_recv.at[m],
                    device_id={"section": below, "dp": me}, device_id_type=MESH,
                ).start()

            wide = result.astype(f32)
            smsg[m, c : c + 1, :] = row_sum(wide)
            smsg[m, chunks + c : chunks + c + 1, :] = row_sum(wide * nrecv[m, :, lanes(c)].astype(f32))

        @pl.when(sec > 0)
        def _():
            to_plane(below, lambda _: smsg.at[m], sbuf.at[m, me], s_send, s_recv.at[m], 0)

        pltpu.make_async_copy(usend.at[m], out.at[0, m, 0], out_sem.at[m]).start()

        pacc[...] += lax.dot_general(
            depth[m], pgs[...], (((0,), (0,)), ((), ())), preferred_element_type=f32
        )
        for c in range(chunks):
            x = x_v[m, :, :, lanes(c)].astype(f32).reshape(rows, LANES)
            active = jnp.maximum(x, 0.0)
            parts = columns_of(dgs[:, lanes(c)], width)[::-1]
            per = kacc.shape[1]
            for i in range(3):
                for j in range(3):
                    moved = (up(parts[j], width), parts[j], down(parts[j], width))[i]
                    r = (3 * i + j) * chunks + c
                    kacc[r // per, r % per : r % per + 1, :] += row_sum(active * moved)
        return 0

    @pl.when(sec == 0)
    def _():
        nrecv[...] = jnp.zeros(nrecv.shape, bf16)

    lax.fori_loop(0, micros, backward, 0)

    for c in range(chunks):
        bgrad[0:1, lanes(c)] = gacc[c : c + 1, :]
        ggrad[0:1, lanes(c)] = gacc[chunks + c : chunks + c + 1, :]

    rs_src[...] = pacc[...].reshape(rs_src.shape).astype(bf16)
    to_plane(sec, lambda peer: rs_src.at[peer], rs_buf.at[me], rs_send, rs_recv, 1)
    to_plane(sec, lambda peer: kacc.at[peer], krs_buf.at[me], ks_send, ks_recv, 1)
    rs_buf[me] = rs_src[me]
    krs_buf[me] = kacc[me]
    wait_bytes(rs_buf.at[pl.ds(0, replicas - 1)], rs_recv)
    ag_src[...] = jnp.sum(rs_buf[...].astype(f32), axis=0).astype(bf16)
    to_plane(sec, lambda _: ag_src, ag_buf.at[me], ag_send, ag_recv, 1)
    wait_bytes(krs_buf.at[pl.ds(0, replicas - 1)], ks_recv)
    kag_src[...] = jnp.sum(krs_buf[...], axis=0)
    to_plane(sec, lambda _: kag_src, kag_buf.at[me], kg_send, kg_recv, 1)
    ag_buf[me] = ag_src[...]
    kag_buf[me] = kag_src[...]
    wait_bytes(kag_buf.at[pl.ds(0, replicas - 1)], kg_recv)
    per = kacc.shape[1]
    for t in range(9):
        for c in range(chunks):
            r = t * chunks + c
            kgrad[0, t // 3, t % 3 : t % 3 + 1, lanes(c)] = kag_buf[r // per, r % per : r % per + 1, :]
    wait_bytes(ag_buf.at[pl.ds(0, replicas - 1)], ag_recv)
    point[0] = ag_buf[...].astype(f32).reshape(channels, channels)

    for m in range(micros):
        pltpu.make_async_copy(usend.at[m], out.at[0, m, 0], out_sem.at[m]).wait()
    wait_bytes(tbuf.at[:, pl.ds(0, replicas - 1)], t_send)

    @pl.when(sec < last)
    def _():
        wait_bytes(nsend, n_send)

    @pl.when(sec == last)
    def _():
        wait_bytes(sbuf.at[:, pl.ds(0, replicas - 1)], o_send)

    @pl.when(sec > 0)
    def _():
        wait_bytes(usend, u_send)
        wait_bytes(sbuf, s_send)

    wait_bytes(rs_buf.at[pl.ds(0, replicas - 1)], rs_send)
    wait_bytes(krs_buf.at[pl.ds(0, replicas - 1)], ks_send)
    wait_bytes(ag_buf.at[pl.ds(0, replicas - 1)], ag_send)
    wait_bytes(kag_buf.at[pl.ds(0, replicas - 1)], kg_send)


def solution(mesh):
    sections, replicas = mesh.shape["section"], mesh.shape["dp"]

    def body(acts, out_grad, depth_kernel, point_weight, bn_gain):
        micros, _, height, width, channels = acts.shape[1:]
        rows = height * width
        chunks = channels // LANES
        share = channels // replicas
        per = -(-9 * chunks // replicas)
        f32, bf16 = jnp.float32, jnp.bfloat16
        image = (micros, height, width, channels)
        flat = (micros, rows, channels)
        vmem, dma = pltpu.VMEM, pltpu.SemaphoreType.DMA
        any_space = pl.BlockSpec(memory_space=pl.ANY)
        in_vmem = pl.BlockSpec(memory_space=pltpu.VMEM)
        return pl.pallas_call(
            functools.partial(kernel, sections, replicas, micros, height, width, channels),
            out_shape=(
                jax.ShapeDtypeStruct(acts.shape, bf16),
                jax.ShapeDtypeStruct((1, channels, channels), f32),
                jax.ShapeDtypeStruct((1, 3, 3, channels), f32),
                jax.ShapeDtypeStruct((1, channels), f32),
                jax.ShapeDtypeStruct((1, channels), f32),
            ),
            in_specs=[any_space, any_space, in_vmem, any_space, in_vmem],
            out_specs=(any_space, in_vmem, in_vmem, in_vmem, in_vmem),
            scratch_shapes=[
                vmem(image, bf16), vmem((channels, channels), bf16), vmem((9, 1, channels), f32),
                vmem(flat, bf16), vmem(flat, f32), vmem(flat, bf16), vmem(flat, bf16),
                vmem(image, bf16), vmem(image, bf16), vmem((rows, channels), bf16), vmem((rows, channels), f32),
                vmem((micros, replicas, 2 * chunks, LANES), f32), vmem((micros, 2 * chunks, LANES), f32),
                vmem((micros, 2 * chunks, LANES), f32),
                vmem((micros, replicas, 2 * chunks, LANES), f32), vmem((micros, 2 * chunks, LANES), f32),
                vmem((micros, 2 * chunks, LANES), f32), vmem((2 * chunks, LANES), f32),
                vmem((channels, channels), f32),
                vmem((replicas, share, channels), bf16), vmem((replicas, share, channels), bf16),
                vmem((share, channels), bf16), vmem((replicas, share, channels), bf16),
                vmem((replicas, per, LANES), f32), vmem((replicas, per, LANES), f32),
                vmem((per, LANES), f32), vmem((replicas, per, LANES), f32),
                dma((micros + 1,)), dma((micros,)), dma((micros,)),
                dma, dma((micros,)), dma, dma((micros,)), dma, dma((micros,)), dma, dma((micros,)), dma,
                dma, dma, dma, dma, dma, dma, dma, dma,
            ],
            compiler_params=pltpu.CompilerParams(collective_id=0, has_side_effects=True),
        )(acts, out_grad, depth_kernel, point_weight, bn_gain)

    return jax.shard_map(
        body,
        mesh=mesh,
        in_specs=(
            P("section", None, "dp", None, None, None),
            P(None, "dp", None, None, None),
            P("section", None, None, None),
            P("section", None, None),
            P("section", None),
        ),
        out_specs=(
            P("section", None, "dp", None, None, None),
            P("section", None, None),
            P("section", None, None, None),
            P("section", None),
            P("section", None),
        ),
        check_vma=False,
    )
```

```python
import functools

import jax
import jax.numpy as jnp
from jax import lax
from jax.experimental import pallas as pl
from jax.experimental.pallas import tpu as pltpu
from jax.sharding import PartitionSpec as P

MESH = pl.DeviceIdType.MESH
epsilon = 1e-05
LANES = 128


def columns_of(x, width):
    rows = x.shape[0]
    at = lax.broadcasted_iota(jnp.int32, x.shape, 0) % width
    before = jnp.where(at == 0, 0.0, pltpu.roll(x, 1, 0))
    after = jnp.where(at == width - 1, 0.0, pltpu.roll(x, rows - 1, 0))
    return before, x, after


def down(x, width):
    return jnp.concatenate([jnp.zeros((width, x.shape[1]), x.dtype), x[:-width]], axis=0)


def up(x, width):
    return jnp.concatenate([x[width:], jnp.zeros((width, x.shape[1]), x.dtype)], axis=0)


def kernel(
    sections, replicas, micros, height, width, channels,
    acts, out_grad, kern, weight, gain,
    out, point, kgrad, ggrad, bgrad,
    x_v, w_v, kf, depth, normed, nsend, nrecv, ubuf, usend, pgs, dgs,
    ones, lows, base, cmsg, crecv,
    sbuf, fmsg, pbuf, smsg, obuf, omsg, tbuf, tmsg, stat, gacc,
    pacc, rs_src, rs_buf, ag_src, ag_buf, kacc, krs_buf, kag_src, kag_buf,
    in_sem, og_sem, out_sem,
    t_send, t_recv, n_send, n_recv, c_send, c_recv, u_send, u_recv, p_send, p_recv, f_send, s_recv, o_send, o_recv,
    rs_send, rs_recv, ag_send, ag_recv, ks_send, ks_recv, kg_send, kg_recv,
):
    f32, bf16 = jnp.float32, jnp.bfloat16
    sec = lax.axis_index("section")
    me = lax.axis_index("dp")
    rows = height * width
    chunks = channels // LANES
    count = replicas * rows
    last = sections - 1
    below = (sec + sections - 1) % sections
    above = (sec + 1) % sections

    def lanes(c):
        return slice(c * LANES, (c + 1) * LANES)

    for m in range(micros):
        pltpu.make_async_copy(acts.at[0, m, 0], x_v.at[m], in_sem.at[m]).start()
        if m == 0:
            pltpu.make_async_copy(weight.at[0], w_v, in_sem.at[micros]).start()

    @pl.when(sec == last)
    def _():
        for m in range(micros):
            pltpu.make_async_copy(out_grad.at[m, 0], ubuf.at[m], og_sem.at[m]).start()

    barrier = pltpu.get_barrier_semaphore()

    def greet(k, _):
        peer = (me + k) % replicas
        pl.semaphore_signal(barrier, inc=1, device_id={"section": below, "dp": peer}, device_id_type=MESH)
        pl.semaphore_signal(barrier, inc=1, device_id={"section": above, "dp": peer}, device_id_type=MESH)

        @pl.when(k > 0)
        def _():
            pl.semaphore_signal(barrier, inc=1, device_id={"section": sec, "dp": peer}, device_id_type=MESH)

        return 0

    lax.fori_loop(0, replicas, greet, 0)

    for i in range(3):
        for j in range(3):
            kf[3 * i + j] = jnp.reshape(kern[0, i, j].astype(f32), (1, channels))
    kacc[...] = jnp.zeros(kacc.shape, f32)
    gacc[...] = jnp.zeros(gacc.shape, f32)
    pacc[...] = jnp.zeros(pacc.shape, f32)

    def tap(i, j, c):
        return kf[3 * i + j, :, lanes(c)]

    def convolve(x, c):
        parts = columns_of(x, width)
        line = [sum(tap(i, j, c) * parts[j] for j in range(3)) for i in range(3)]
        return down(line[0], width) + line[1] + up(line[2], width)

    def to_plane(section, src, dst, send, recv, first):
        def one(k, _):
            peer = (me + k) % replicas
            pltpu.make_async_remote_copy(
                src_ref=src(peer), dst_ref=dst, send_sem=send, recv_sem=recv,
                device_id={"section": section, "dp": peer}, device_id_type=MESH,
            ).start()
            return 0

        lax.fori_loop(first, replicas, one, 0)

    def wait_bytes(ref, sem):
        pltpu.make_async_copy(ref, ref, sem).wait()

    def row_sum(x):
        return jnp.sum(x, axis=0, keepdims=True)

    def forward(m, _):
        pltpu.make_async_copy(acts.at[0, m, 0], x_v.at[m], in_sem.at[m]).wait()
        for c in range(chunks):
            x = x_v[m, :, :, lanes(c)].astype(f32).reshape(rows, LANES)
            depth[m, :, lanes(c)] = convolve(jnp.maximum(x, 0.0), c).astype(bf16)

        @pl.when(m == 0)
        def _():
            pltpu.make_async_copy(weight.at[0], w_v, in_sem.at[micros]).wait()

        normed[m] = jnp.dot(depth[m], w_v[...], preferred_element_type=f32)
        for c in range(chunks):
            pre = normed[m, :, lanes(c)]
            tmsg[m, c : c + 1, :] = row_sum(pre)
            tmsg[m, chunks + c : chunks + c + 1, :] = row_sum(pre * pre)
            cmsg[m, c : c + 1, :] = tmsg[m, c : c + 1, :] / rows
            nsend[m, :, lanes(c)] = (pre - cmsg[m, c : c + 1, :]).astype(bf16)

        @pl.when(m == 0)
        def _():
            pl.semaphore_wait(barrier, 3 * replicas - 1)

        to_plane(sec, lambda _: tmsg.at[m], tbuf.at[m, me], t_send, t_recv.at[m], 1)
        tbuf[m, me] = tmsg[m]

        @pl.when(sec < last)
        def _():
            for src, dst, send, recv in ((cmsg, crecv, c_send, c_recv), (nsend, nrecv, n_send, n_recv)):
                pltpu.make_async_remote_copy(
                    src_ref=src.at[m], dst_ref=dst.at[m], send_sem=send, recv_sem=recv.at[m],
                    device_id={"section": above, "dp": me}, device_id_type=MESH,
                ).start()

        @pl.when(sec == last)
        def _():
            pltpu.make_async_copy(out_grad.at[m, 0], ubuf.at[m], og_sem.at[m]).wait()
            for c in range(chunks):
                u = ubuf[m, :, :, lanes(c)].astype(f32).reshape(rows, LANES)
                omsg[m, c : c + 1, :] = row_sum(u)
                omsg[m, chunks + c : chunks + c + 1, :] = row_sum(u * normed[m, :, lanes(c)])
            to_plane(sec, lambda _: omsg.at[m], obuf.at[m, me], o_send, o_recv.at[m], 1)
            obuf[m, me] = omsg[m]

        return 0

    lax.fori_loop(0, micros, forward, 0)

    def prepare(m):
        wait_bytes(tbuf.at[m, pl.ds(0, replicas - 1)], t_recv.at[m])
        total = jnp.sum(tbuf[m], axis=0) / count
        center = total[:chunks]
        inv_std = lax.rsqrt(total[chunks:] - center * center + epsilon)
        stat[0:chunks, :] = center
        stat[chunks:, :] = inv_std
        for c in range(chunks):
            normed[m, :, lanes(c)] = (normed[m, :, lanes(c)] - center[c : c + 1]) * inv_std[c : c + 1]

        @pl.when(sec > 0)
        def _():
            wait_bytes(nrecv.at[m], n_recv.at[m])
            wait_bytes(crecv.at[m], c_recv.at[m])
            for c in range(chunks):
                x = x_v[m, :, :, lanes(c)].astype(f32).reshape(rows, LANES)
                low = nrecv[m, :, lanes(c)].astype(f32)
                ones[:, lanes(c)] = convolve(jnp.where(x > 0, 1.0, 0.0), c)
                lows[:, lanes(c)] = convolve(jnp.where(x > 0, low, 0.0), c)

    def critical(m):
        @pl.when(sec < last)
        def _():
            wait_bytes(ubuf.at[m], u_recv.at[m])

        @pl.when(sec > 0)
        def _():
            for c in range(chunks):
                u = ubuf[m, :, :, lanes(c)].astype(f32).reshape(rows, LANES)
                base[c : c + 1, :] = row_sum(u)
                base[chunks + c : chunks + c + 1, :] = row_sum(u * nrecv[m, :, lanes(c)].astype(f32))

        @pl.when(sec == last)
        def _():
            wait_bytes(obuf.at[m, pl.ds(0, replicas - 1)], o_recv.at[m])
            sbuf[m] = jnp.sum(obuf[m], axis=0)

        @pl.when(sec < last)
        def _():
            wait_bytes(sbuf.at[m], s_recv.at[m])

        total = sbuf[m]
        center, inv_std = stat[0:chunks, :], stat[chunks:, :]
        sum_grad = total[:chunks]
        cross = inv_std * (total[chunks:] - center * sum_grad)
        gacc[0:chunks, :] += sum_grad
        gacc[chunks:, :] += cross
        for c in range(chunks):
            scale = gain[0:1, lanes(c)] * inv_std[c : c + 1]
            shift = scale * sum_grad[c : c + 1] / count
            slope = scale * cross[c : c + 1] / count
            u = ubuf[m, :, :, lanes(c)].astype(f32).reshape(rows, LANES)
            pgs[:, lanes(c)] = (scale * u - shift - slope * normed[m, :, lanes(c)]).astype(bf16)
        dgs[...] = lax.dot_general(pgs[...], w_v[...], (((1,), (1,)), ((), ())), preferred_element_type=f32)

        @pl.when(sec > 0)
        def _():
            for c in range(chunks):
                grad = dgs[:, lanes(c)]
                plain = base[c : c + 1, :] + row_sum(grad * ones[:, lanes(c)])
                mixed = base[chunks + c : chunks + c + 1, :] + row_sum(grad * lows[:, lanes(c)])
                smsg[m, c : c + 1, :] = plain
                smsg[m, chunks + c : chunks + c + 1, :] = mixed + crecv[m, c : c + 1, :] * plain
            to_plane(sec, lambda _: smsg.at[m], pbuf.at[m, me], p_send, p_recv.at[m], 1)
            pbuf[m, me] = smsg[m]

        for c in range(chunks):
            parts = columns_of(dgs[:, lanes(c)], width)[::-1]
            line = [sum(tap(i, j, c) * parts[j] for j in range(3)) for i in range(3)]
            back = up(line[0], width) + line[1] + down(line[2], width)
            u = ubuf[m, :, :, lanes(c)].astype(f32).reshape(rows, LANES)
            x = x_v[m, :, :, lanes(c)].astype(f32).reshape(rows, LANES)
            result = (u + jnp.where(x > 0, back, 0.0)).astype(bf16)
            usend[m, :, :, lanes(c)] = result.reshape(height, width, LANES)

            @pl.when(sec > 0)
            def _():
                pltpu.make_async_remote_copy(
                    src_ref=usend.at[m, :, :, pl.ds(c * LANES, LANES)],
                    dst_ref=ubuf.at[m, :, :, pl.ds(c * LANES, LANES)],
                    send_sem=u_send, recv_sem=u_recv.at[m],
                    device_id={"section": below, "dp": me}, device_id_type=MESH,
                ).start()

        pltpu.make_async_copy(usend.at[m], out.at[0, m, 0], out_sem.at[m]).start()

    def hand_down(m):
        @pl.when(sec > 0)
        def _():
            wait_bytes(pbuf.at[m, pl.ds(0, replicas - 1)], p_recv.at[m])
            fmsg[m] = jnp.sum(pbuf[m], axis=0)
            pltpu.make_async_remote_copy(
                src_ref=fmsg.at[m], dst_ref=sbuf.at[m], send_sem=f_send, recv_sem=s_recv.at[m],
                device_id={"section": below, "dp": me}, device_id_type=MESH,
            ).start()

    def weights(m):
        pacc[...] += lax.dot_general(
            depth[m], pgs[...], (((0,), (0,)), ((), ())), preferred_element_type=f32
        )
        per = kacc.shape[1]
        for c in range(chunks):
            x = x_v[m, :, :, lanes(c)].astype(f32).reshape(rows, LANES)
            active = jnp.maximum(x, 0.0)
            parts = columns_of(dgs[:, lanes(c)], width)[::-1]
            for i in range(3):
                for j in range(3):
                    moved = (up(parts[j], width), parts[j], down(parts[j], width))[i]
                    r = (3 * i + j) * chunks + c
                    kacc[r // per, r % per : r % per + 1, :] += row_sum(active * moved)

    def backward(m, _):
        prepare(m)
        critical(m)
        weights(m)
        hand_down(m)
        return 0

    lax.fori_loop(0, micros, backward, 0)

    for c in range(chunks):
        bgrad[0:1, lanes(c)] = gacc[c : c + 1, :]
        ggrad[0:1, lanes(c)] = gacc[chunks + c : chunks + c + 1, :]

    rs_src[...] = pacc[...].reshape(rs_src.shape).astype(bf16)
    to_plane(sec, lambda peer: rs_src.at[peer], rs_buf.at[me], rs_send, rs_recv, 1)
    to_plane(sec, lambda peer: kacc.at[peer], krs_buf.at[me], ks_send, ks_recv, 1)
    rs_buf[me] = rs_src[me]
    krs_buf[me] = kacc[me]
    wait_bytes(rs_buf.at[pl.ds(0, replicas - 1)], rs_recv)
    ag_src[...] = jnp.sum(rs_buf[...].astype(f32), axis=0).astype(bf16)
    to_plane(sec, lambda _: ag_src, ag_buf.at[me], ag_send, ag_recv, 1)
    wait_bytes(krs_buf.at[pl.ds(0, replicas - 1)], ks_recv)
    kag_src[...] = jnp.sum(krs_buf[...], axis=0)
    to_plane(sec, lambda _: kag_src, kag_buf.at[me], kg_send, kg_recv, 1)
    ag_buf[me] = ag_src[...]
    kag_buf[me] = kag_src[...]
    wait_bytes(kag_buf.at[pl.ds(0, replicas - 1)], kg_recv)
    per = kacc.shape[1]
    for t in range(9):
        for c in range(chunks):
            r = t * chunks + c
            kgrad[0, t // 3, t % 3 : t % 3 + 1, lanes(c)] = kag_buf[r // per, r % per : r % per + 1, :]
    wait_bytes(ag_buf.at[pl.ds(0, replicas - 1)], ag_recv)
    point[0] = ag_buf[...].reshape(channels, channels)

    for m in range(micros):
        pltpu.make_async_copy(usend.at[m], out.at[0, m, 0], out_sem.at[m]).wait()
    wait_bytes(tbuf.at[:, pl.ds(0, replicas - 1)], t_send)

    @pl.when(sec < last)
    def _():
        wait_bytes(nsend, n_send)
        wait_bytes(cmsg, c_send)

    @pl.when(sec == last)
    def _():
        wait_bytes(obuf.at[:, pl.ds(0, replicas - 1)], o_send)

    @pl.when(sec > 0)
    def _():
        wait_bytes(usend, u_send)
        wait_bytes(pbuf.at[:, pl.ds(0, replicas - 1)], p_send)
        wait_bytes(fmsg, f_send)

    wait_bytes(rs_buf.at[pl.ds(0, replicas - 1)], rs_send)
    wait_bytes(krs_buf.at[pl.ds(0, replicas - 1)], ks_send)
    wait_bytes(ag_buf.at[pl.ds(0, replicas - 1)], ag_send)
    wait_bytes(kag_buf.at[pl.ds(0, replicas - 1)], kg_send)


def solution(mesh):
    sections, replicas = mesh.shape["section"], mesh.shape["dp"]

    def body(acts, out_grad, depth_kernel, point_weight, bn_gain):
        micros, _, height, width, channels = acts.shape[1:]
        rows = height * width
        chunks = channels // LANES
        share = channels // replicas
        per = -(-9 * chunks // replicas)
        f32, bf16 = jnp.float32, jnp.bfloat16
        image = (micros, height, width, channels)
        flat = (micros, rows, channels)
        sums = (2 * chunks, LANES)
        vmem, dma = pltpu.VMEM, pltpu.SemaphoreType.DMA
        any_space = pl.BlockSpec(memory_space=pl.ANY)
        in_vmem = pl.BlockSpec(memory_space=pltpu.VMEM)
        grads, point, kgrad, ggrad, bgrad = pl.pallas_call(
            functools.partial(kernel, sections, replicas, micros, height, width, channels),
            out_shape=(
                jax.ShapeDtypeStruct(acts.shape, bf16),
                jax.ShapeDtypeStruct((1, channels, channels), bf16),
                jax.ShapeDtypeStruct((1, 3, 3, channels), f32),
                jax.ShapeDtypeStruct((1, channels), f32),
                jax.ShapeDtypeStruct((1, channels), f32),
            ),
            in_specs=[any_space, any_space, in_vmem, any_space, in_vmem],
            out_specs=(any_space, in_vmem, in_vmem, in_vmem, in_vmem),
            scratch_shapes=[
                vmem(image, bf16), vmem((channels, channels), bf16), vmem((9, 1, channels), f32),
                vmem(flat, bf16), vmem(flat, f32), vmem(flat, bf16), vmem(flat, bf16),
                vmem(image, bf16), vmem(image, bf16), vmem((rows, channels), bf16), vmem((rows, channels), f32),
                vmem((rows, channels), f32), vmem((rows, channels), f32), vmem(sums, f32),
                vmem((micros, chunks, LANES), f32), vmem((micros, chunks, LANES), f32),
                vmem((micros, *sums), f32), vmem((micros, *sums), f32),
                vmem((micros, replicas, *sums), f32), vmem((micros, *sums), f32),
                vmem((micros, replicas, *sums), f32), vmem((micros, *sums), f32),
                vmem((micros, replicas, *sums), f32), vmem((micros, *sums), f32),
                vmem(sums, f32), vmem(sums, f32),
                vmem((channels, channels), f32),
                vmem((replicas, share, channels), bf16), vmem((replicas, share, channels), bf16),
                vmem((share, channels), bf16), vmem((replicas, share, channels), bf16),
                vmem((replicas, per, LANES), f32), vmem((replicas, per, LANES), f32),
                vmem((per, LANES), f32), vmem((replicas, per, LANES), f32),
                dma((micros + 1,)), dma((micros,)), dma((micros,)),
                *[dma, dma((micros,))] * 7,
                dma, dma, dma, dma, dma, dma, dma, dma,
            ],
            compiler_params=pltpu.CompilerParams(collective_id=0, has_side_effects=True),
        )(acts, out_grad, depth_kernel, point_weight, bn_gain)
        return grads, point.astype(f32), kgrad, ggrad, bgrad

    return jax.shard_map(
        body,
        mesh=mesh,
        in_specs=(
            P("section", None, "dp", None, None, None),
            P(None, "dp", None, None, None),
            P("section", None, None, None),
            P("section", None, None),
            P("section", None),
        ),
        out_specs=(
            P("section", None, "dp", None, None, None),
            P("section", None, None),
            P("section", None, None, None),
            P("section", None),
            P("section", None),
        ),
        check_vma=False,
    )
```

```python
import functools

import jax
import jax.numpy as jnp
from jax import lax
from jax.experimental import pallas as pl
from jax.experimental.pallas import tpu as pltpu
from jax.sharding import PartitionSpec as P

MESH = pl.DeviceIdType.MESH
epsilon = 1e-05
LANES = 128
REACH = 2


def columns_of(x, width):
    rows = x.shape[0]
    at = lax.broadcasted_iota(jnp.int32, x.shape, 0) % width
    before = jnp.where(at == 0, 0.0, pltpu.roll(x, 1, 0))
    after = jnp.where(at == width - 1, 0.0, pltpu.roll(x, rows - 1, 0))
    return before, x, after


def down(x, width):
    return jnp.concatenate([jnp.zeros((width, x.shape[1]), x.dtype), x[:-width]], axis=0)


def up(x, width):
    return jnp.concatenate([x[width:], jnp.zeros((width, x.shape[1]), x.dtype)], axis=0)


def ring(a, n):
    return min(a, n - a)


def offsets(ys, xs, reach):
    every = [(y, x, c) for y in range(ys) for x in range(xs) for c in range(2) if (y, x, c) != (0, 0, 0)]
    every.sort(key=lambda o: -(ring(o[0], ys) + ring(o[1], xs)))
    far = [o for o in every if ring(o[0], ys) + ring(o[1], xs) > reach]
    return far, [o for o in every if o not in far]


def kernel(
    ys, xs, far, near,
    sections, replicas, micros, height, width, channels,
    acts, out_grad, kern, weight, gain,
    out, point, kgrad, ggrad, bgrad,
    x_v, w_v, kf, depth, normed, nsend, nrecv, ubuf, usend, pgs, dgs,
    ones, lows, base, cmsg, crecv,
    dmsg, dbuf, sbuf, fmsg, pbuf, smsg, obuf, omsg, tbuf, tmsg, stat, gacc,
    pacc, pair_src, pair_buf, rs_src, rs_buf, ag_src, ag_buf, kacc, krs_buf, kag_src, kag_buf,
    in_sem, og_sem, out_sem,
    t_send, t_recv, n_send, n_recv, c_send, c_recv, u_send, u_recv, p_send, p_recv, f_send, s_recv, o_send, o_recv,
    d_send, d_recv, w_send, w_recv, rs_send, rs_recv, ag_send, ag_recv, m_send, m_recv, ks_send, ks_recv, kg_send, kg_recv,
):
    f32, bf16 = jnp.float32, jnp.bfloat16
    sec = lax.axis_index("section")
    me = lax.axis_index("dp")
    rows = height * width
    chunks = channels // LANES
    count = replicas * rows
    last = sections - 1
    below = (sec + sections - 1) % sections
    above = (sec + 1) % sections

    def lanes(c):
        return slice(c * LANES, (c + 1) * LANES)

    for m in range(micros):
        pltpu.make_async_copy(acts.at[0, m, 0], x_v.at[m], in_sem.at[m]).start()
        if m == 0:
            pltpu.make_async_copy(weight.at[0], w_v, in_sem.at[micros]).start()

    @pl.when(sec == last)
    def _():
        for m in range(micros):
            pltpu.make_async_copy(out_grad.at[m, 0], ubuf.at[m], og_sem.at[m]).start()

    barrier = pltpu.get_barrier_semaphore()

    def greet(k, _):
        peer = (me + k) % replicas
        pl.semaphore_signal(barrier, inc=1, device_id={"section": below, "dp": peer}, device_id_type=MESH)
        pl.semaphore_signal(barrier, inc=1, device_id={"section": above, "dp": peer}, device_id_type=MESH)

        @pl.when(k > 0)
        def _():
            pl.semaphore_signal(barrier, inc=1, device_id={"section": sec, "dp": peer}, device_id_type=MESH)

        return 0

    lax.fori_loop(0, replicas, greet, 0)

    for i in range(3):
        for j in range(3):
            kf[3 * i + j] = jnp.reshape(kern[0, i, j].astype(f32), (1, channels))
    kacc[...] = jnp.zeros(kacc.shape, f32)
    gacc[...] = jnp.zeros(gacc.shape, f32)
    pacc[...] = jnp.zeros(pacc.shape, f32)

    def tap(i, j, c):
        return kf[3 * i + j, :, lanes(c)]

    def convolve(x, c):
        parts = columns_of(x, width)
        line = [sum(tap(i, j, c) * parts[j] for j in range(3)) for i in range(3)]
        return down(line[0], width) + line[1] + up(line[2], width)

    core, at_x, at_y = me % 2, (me // 2) % xs, me // (2 * xs)

    def device_at(offset):
        dy, dx, dc = offset
        return (((at_y + dy) % ys) * xs + (at_x + dx) % xs) * 2 + (core + dc) % 2

    def to_peer(src, dst, send, recv, section, peer):
        pltpu.make_async_remote_copy(
            src_ref=src, dst_ref=dst, send_sem=send, recv_sem=recv,
            device_id={"section": section, "dp": peer}, device_id_type=MESH,
        ).start()

    def to_plane(section, src, dst, send, recv, first):
        def one(k, _):
            peer = (me + k) % replicas
            pltpu.make_async_remote_copy(
                src_ref=src(peer), dst_ref=dst, send_sem=send, recv_sem=recv,
                device_id={"section": section, "dp": peer}, device_id_type=MESH,
            ).start()
            return 0

        lax.fori_loop(first, replicas, one, 0)

    def wait_bytes(ref, sem):
        pltpu.make_async_copy(ref, ref, sem).wait()

    def row_sum(x):
        return jnp.sum(x, axis=0, keepdims=True)

    def forward(m, _):
        pltpu.make_async_copy(acts.at[0, m, 0], x_v.at[m], in_sem.at[m]).wait()
        for c in range(chunks):
            x = x_v[m, :, :, lanes(c)].astype(f32).reshape(rows, LANES)
            depth[m, :, lanes(c)] = convolve(jnp.maximum(x, 0.0), c).astype(bf16)

        @pl.when(m == 0)
        def _():
            pltpu.make_async_copy(weight.at[0], w_v, in_sem.at[micros]).wait()

        normed[m] = jnp.dot(depth[m], w_v[...], preferred_element_type=f32)
        for c in range(chunks):
            pre = normed[m, :, lanes(c)]
            tmsg[m, c : c + 1, :] = row_sum(pre)
            tmsg[m, chunks + c : chunks + c + 1, :] = row_sum(pre * pre)
            cmsg[m, c : c + 1, :] = tmsg[m, c : c + 1, :] / rows
            nsend[m, :, lanes(c)] = (pre - cmsg[m, c : c + 1, :]).astype(bf16)

        @pl.when(m == 0)
        def _():
            pl.semaphore_wait(barrier, 3 * replicas - 1)

        @pl.when(sec < last)
        def _():
            for src, dst, send, recv in ((cmsg, crecv, c_send, c_recv), (nsend, nrecv, n_send, n_recv)):
                pltpu.make_async_remote_copy(
                    src_ref=src.at[m], dst_ref=dst.at[m], send_sem=send, recv_sem=recv.at[m],
                    device_id={"section": above, "dp": me}, device_id_type=MESH,
                ).start()

        to_plane(sec, lambda _: tmsg.at[m], tbuf.at[m, me], t_send, t_recv.at[m], 1)
        tbuf[m, me] = tmsg[m]

        @pl.when(sec == last)
        def _():
            pltpu.make_async_copy(out_grad.at[m, 0], ubuf.at[m], og_sem.at[m]).wait()
            for c in range(chunks):
                u = ubuf[m, :, :, lanes(c)].astype(f32).reshape(rows, LANES)
                omsg[m, c : c + 1, :] = row_sum(u)
                omsg[m, chunks + c : chunks + c + 1, :] = row_sum(u * normed[m, :, lanes(c)])
            to_plane(sec, lambda _: omsg.at[m], obuf.at[m, me], o_send, o_recv.at[m], 1)
            obuf[m, me] = omsg[m]

        return 0

    lax.fori_loop(0, micros, forward, 0)

    def prepare(m):
        wait_bytes(tbuf.at[m, pl.ds(0, replicas - 1)], t_recv.at[m])
        total = jnp.sum(tbuf[m], axis=0) / count
        center = total[:chunks]
        inv_std = lax.rsqrt(total[chunks:] - center * center + epsilon)
        stat[0:chunks, :] = center
        stat[chunks:, :] = inv_std
        for c in range(chunks):
            normed[m, :, lanes(c)] = (normed[m, :, lanes(c)] - center[c : c + 1]) * inv_std[c : c + 1]

        @pl.when(sec > 0)
        def _():
            for c in range(chunks):
                x = x_v[m, :, :, lanes(c)].astype(f32).reshape(rows, LANES)
                ones[:, lanes(c)] = convolve(jnp.where(x > 0, 1.0, 0.0), c)
            wait_bytes(nrecv.at[m], n_recv.at[m])
            wait_bytes(crecv.at[m], c_recv.at[m])
            for c in range(chunks):
                x = x_v[m, :, :, lanes(c)].astype(f32).reshape(rows, LANES)
                low = nrecv[m, :, lanes(c)].astype(f32)
                lows[:, lanes(c)] = convolve(jnp.where(x > 0, low, 0.0), c)

    def critical(m):
        @pl.when(sec < last)
        def _():
            wait_bytes(ubuf.at[m], u_recv.at[m])

        @pl.when(sec > 0)
        def _():
            for c in range(chunks):
                u = ubuf[m, :, :, lanes(c)].astype(f32).reshape(rows, LANES)
                base[c : c + 1, :] = row_sum(u)
                base[chunks + c : chunks + c + 1, :] = row_sum(u * nrecv[m, :, lanes(c)].astype(f32))

        @pl.when(sec == last)
        def _():
            wait_bytes(obuf.at[m, pl.ds(0, replicas - 1)], o_recv.at[m])
            sbuf[m] = jnp.sum(obuf[m], axis=0)
            dbuf[m] = jnp.zeros(dbuf.shape[1:], bf16)

        @pl.when(sec < last)
        def _():
            if far:
                wait_bytes(dbuf.at[m], d_recv.at[m])
            wait_bytes(sbuf.at[m], s_recv.at[m])

        total = sbuf[m]
        if far:
            total = total + jnp.sum(dbuf[m].astype(f32), axis=0)
        center, inv_std = stat[0:chunks, :], stat[chunks:, :]
        sum_grad = total[:chunks]
        cross = inv_std * (total[chunks:] - center * sum_grad)
        gacc[0:chunks, :] += sum_grad
        gacc[chunks:, :] += cross
        for c in range(chunks):
            scale = gain[0:1, lanes(c)] * inv_std[c : c + 1]
            shift = scale * sum_grad[c : c + 1] / count
            slope = scale * cross[c : c + 1] / count
            u = ubuf[m, :, :, lanes(c)].astype(f32).reshape(rows, LANES)
            pgs[:, lanes(c)] = (scale * u - shift - slope * normed[m, :, lanes(c)]).astype(bf16)
        dgs[...] = lax.dot_general(pgs[...], w_v[...], (((1,), (1,)), ((), ())), preferred_element_type=f32)

        @pl.when(sec > 0)
        def _():
            for c in range(chunks):
                grad = dgs[:, lanes(c)]
                plain = base[c : c + 1, :] + row_sum(grad * ones[:, lanes(c)])
                mixed = base[chunks + c : chunks + c + 1, :] + row_sum(grad * lows[:, lanes(c)])
                smsg[m, c : c + 1, :] = plain
                smsg[m, chunks + c : chunks + c + 1, :] = mixed + crecv[m, c : c + 1, :] * plain
            if far:
                dmsg[m] = smsg[m].astype(bf16)
            for k, o in enumerate(far):
                to_peer(dmsg.at[m], dbuf.at[m, k], d_send, d_recv.at[m], below, device_at(o))
            for k, o in enumerate(near):
                to_peer(smsg.at[m], pbuf.at[m, k], p_send, p_recv.at[m], sec, device_at(o))

        for c in range(chunks):
            parts = columns_of(dgs[:, lanes(c)], width)[::-1]
            line = [sum(tap(i, j, c) * parts[j] for j in range(3)) for i in range(3)]
            back = up(line[0], width) + line[1] + down(line[2], width)
            u = ubuf[m, :, :, lanes(c)].astype(f32).reshape(rows, LANES)
            x = x_v[m, :, :, lanes(c)].astype(f32).reshape(rows, LANES)
            result = (u + jnp.where(x > 0, back, 0.0)).astype(bf16)
            usend[m, :, :, lanes(c)] = result.reshape(height, width, LANES)

            @pl.when(sec > 0)
            def _():
                pltpu.make_async_remote_copy(
                    src_ref=usend.at[m, :, :, pl.ds(c * LANES, LANES)],
                    dst_ref=ubuf.at[m, :, :, pl.ds(c * LANES, LANES)],
                    send_sem=u_send, recv_sem=u_recv.at[m],
                    device_id={"section": below, "dp": me}, device_id_type=MESH,
                ).start()

        pltpu.make_async_copy(usend.at[m], out.at[0, m, 0], out_sem.at[m]).start()

    def hand_down(m):
        @pl.when(sec > 0)
        def _():
            wait_bytes(pbuf.at[m], p_recv.at[m])
            fmsg[m] = smsg[m] + jnp.sum(pbuf[m], axis=0)
            to_peer(fmsg.at[m], sbuf.at[m], f_send, s_recv.at[m], below, me)

    def weights(m):
        pacc[...] += lax.dot_general(
            depth[m], pgs[...], (((0,), (0,)), ((), ())), preferred_element_type=f32
        )
        per = kacc.shape[1]
        for c in range(chunks):
            x = x_v[m, :, :, lanes(c)].astype(f32).reshape(rows, LANES)
            active = jnp.maximum(x, 0.0)
            parts = columns_of(dgs[:, lanes(c)], width)[::-1]
            for i in range(3):
                for j in range(3):
                    moved = (up(parts[j], width), parts[j], down(parts[j], width))[i]
                    r = (3 * i + j) * chunks + c
                    kacc[r // per, r % per : r % per + 1, :] += row_sum(active * moved)

    def backward(m, _):
        critical(m)
        weights(m)

        @pl.when(m < micros - 1)
        def _():
            prepare(m + 1)

        hand_down(m)
        return 0

    prepare(0)
    lax.fori_loop(0, micros, backward, 0)

    per = kacc.shape[1]
    for k in range(2 * chunks):
        r = 9 * chunks + k
        kacc[r // per, r % per : r % per + 1, :] = jnp.where(me == 0, gacc[k : k + 1, :], 0.0)

    half = channels // 2
    chip, mate = me // 2, me + 1 - 2 * core
    chips = replicas // 2
    others = [o for o in offsets(ys, xs, 0)[0] if o[2] == 0]
    mine, its = pl.ds(pl.multiple_of(core * half, half), half), pl.ds(pl.multiple_of((1 - core) * half, half), half)
    pair_src[...] = pacc[its, :].astype(bf16)
    to_peer(pair_src, pair_buf, w_send, w_recv, sec, mate)
    to_plane(sec, lambda peer: kacc.at[peer], krs_buf.at[me], ks_send, ks_recv, 1)
    krs_buf[me] = kacc[me]
    wait_bytes(pair_buf, w_recv)
    rs_src[...] = (pacc[mine, :] + pair_buf[...].astype(f32)).astype(bf16).reshape(rs_src.shape)
    for o in others:
        peer = device_at(o)
        to_peer(rs_src.at[peer // 2], rs_buf.at[chip], rs_send, rs_recv, sec, peer)
    rs_buf[chip] = rs_src[chip]
    wait_bytes(krs_buf.at[pl.ds(0, replicas - 1)], ks_recv)
    kag_src[...] = jnp.sum(krs_buf[...], axis=0)
    wait_bytes(rs_buf.at[pl.ds(0, chips - 1)], rs_recv)
    ag_src[...] = jnp.sum(rs_buf[...].astype(f32), axis=0).astype(bf16)
    for k, o in enumerate(others):
        to_peer(ag_src, ag_buf.at[core, chip], ag_send, ag_recv.at[k], sec, device_at(o))
    to_peer(ag_src, ag_buf.at[core, chip], ag_send, m_recv, sec, mate)
    ag_buf[core, chip] = ag_src[...]
    to_plane(sec, lambda _: kag_src, kag_buf.at[me], kg_send, kg_recv, 1)
    kag_buf[me] = kag_src[...]
    for k, o in reversed(list(enumerate(others))):
        source = device_at((-o[0], -o[1], 0)) // 2
        wait_bytes(ag_src, ag_recv.at[k])
        to_peer(ag_buf.at[core, source], ag_buf.at[core, source], m_send, m_recv, sec, mate)
    wait_bytes(kag_buf.at[pl.ds(0, replicas - 1)], kg_recv)
    for t in range(9):
        for c in range(chunks):
            r = t * chunks + c
            kgrad[0, t // 3, t % 3 : t % 3 + 1, lanes(c)] = kag_buf[r // per, r % per : r % per + 1, :]
    for c in range(chunks):
        for at, ref in ((9, bgrad), (10, ggrad)):
            r = at * chunks + c
            ref[0:1, lanes(c)] = kag_buf[r // per, r % per : r % per + 1, :]
    wait_bytes(ag_buf.at[0], m_recv)
    point[0] = ag_buf[...].reshape(channels, channels)

    for m in range(micros):
        pltpu.make_async_copy(usend.at[m], out.at[0, m, 0], out_sem.at[m]).wait()
    wait_bytes(tbuf.at[:, pl.ds(0, replicas - 1)], t_send)

    @pl.when(sec < last)
    def _():
        wait_bytes(nsend, n_send)
        wait_bytes(cmsg, c_send)

    @pl.when(sec == last)
    def _():
        wait_bytes(obuf.at[:, pl.ds(0, replicas - 1)], o_send)

    @pl.when(sec > 0)
    def _():
        wait_bytes(usend, u_send)
        wait_bytes(pbuf, p_send)
        if far:
            wait_bytes(dbuf, d_send)
        wait_bytes(fmsg, f_send)

    wait_bytes(pair_src, w_send)
    wait_bytes(rs_buf.at[pl.ds(0, chips - 1)], rs_send)
    wait_bytes(rs_buf.at[pl.ds(0, chips - 1)], m_send)
    wait_bytes(krs_buf.at[pl.ds(0, replicas - 1)], ks_send)
    wait_bytes(rs_buf, ag_send)
    wait_bytes(kag_buf.at[pl.ds(0, replicas - 1)], kg_send)


def finish(grads, point, kgrad, ggrad, bgrad, grads_out, point_out, kgrad_out, ggrad_out, bgrad_out, held, narrow, wide, in_sem, out_sem, p_in, p_out):
    parts = grads.shape[1]
    share = point.shape[1] // parts

    def copies(m):
        at = pl.ds(m * share, share)
        return (
            pltpu.make_async_copy(point.at[0, at], narrow.at[at], p_in.at[m]),
            pltpu.make_async_copy(grads.at[0, m], held.at[m], in_sem.at[m]),
            pltpu.make_async_copy(wide.at[at], point_out.at[0, at], p_out.at[m]),
            pltpu.make_async_copy(held.at[m], grads_out.at[0, m], out_sem.at[m]),
        )

    for m in range(parts):
        copies(m)[0].start()
        copies(m)[1].start()
    for t in range(9):
        kgrad_out[t // 3, t % 3, 0:1, :] = kgrad[0, t // 3, t % 3 : t % 3 + 1, :]
    ggrad_out[...] = ggrad[...]
    bgrad_out[...] = bgrad[...]
    for m in range(parts):
        at = slice(m * share, (m + 1) * share)
        point_in, grads_in, point_back, grads_back = copies(m)
        point_in.wait()
        wide[at, :] = narrow[at, :].astype(jnp.float32)
        point_back.start()
        grads_in.wait()
        grads_back.start()
    for m in range(parts):
        copies(m)[2].wait()
        copies(m)[3].wait()


def solution(mesh):
    sections, replicas = mesh.shape["section"], mesh.shape["dp"]
    chips = replicas // 2
    ys = max(y for y in range(1, chips + 1) if y * y <= chips and chips % y == 0)
    xs = chips // ys
    far, near = offsets(ys, xs, REACH)

    def body(acts, out_grad, depth_kernel, point_weight, bn_gain):
        micros, _, height, width, channels = acts.shape[1:]
        rows = height * width
        chunks = channels // LANES
        share = channels // replicas
        per = -(-11 * chunks // replicas)
        f32, bf16 = jnp.float32, jnp.bfloat16
        image = (micros, height, width, channels)
        flat = (micros, rows, channels)
        sums = (2 * chunks, LANES)
        vmem, dma = pltpu.VMEM, pltpu.SemaphoreType.DMA
        any_space = pl.BlockSpec(memory_space=pl.ANY)
        in_vmem = pl.BlockSpec(memory_space=pltpu.VMEM)
        results = pl.pallas_call(
            functools.partial(kernel, ys, xs, far, near, sections, replicas, micros, height, width, channels),
            out_shape=(
                jax.ShapeDtypeStruct(acts.shape, bf16),
                jax.ShapeDtypeStruct((1, channels, channels), bf16),
                jax.ShapeDtypeStruct((1, 3, 3, channels), f32),
                jax.ShapeDtypeStruct((1, channels), f32),
                jax.ShapeDtypeStruct((1, channels), f32),
            ),
            in_specs=[any_space, any_space, in_vmem, any_space, in_vmem],
            out_specs=(any_space, in_vmem, in_vmem, in_vmem, in_vmem),
            scratch_shapes=[
                vmem(image, bf16), vmem((channels, channels), bf16), vmem((9, 1, channels), f32),
                vmem(flat, bf16), vmem(flat, f32), vmem(flat, bf16), vmem(flat, bf16),
                vmem(image, bf16), vmem(image, bf16), vmem((rows, channels), bf16), vmem((rows, channels), f32),
                vmem((rows, channels), f32), vmem((rows, channels), f32), vmem(sums, f32),
                vmem((micros, chunks, LANES), f32), vmem((micros, chunks, LANES), f32),
                vmem((micros, *sums), bf16), vmem((micros, max(len(far), 1), *sums), bf16),
                vmem((micros, *sums), f32), vmem((micros, *sums), f32),
                vmem((micros, len(near), *sums), f32), vmem((micros, *sums), f32),
                vmem((micros, replicas, *sums), f32), vmem((micros, *sums), f32),
                vmem((micros, replicas, *sums), f32), vmem((micros, *sums), f32),
                vmem(sums, f32), vmem(sums, f32),
                vmem((channels, channels), f32),
                vmem((channels // 2, channels), bf16), vmem((channels // 2, channels), bf16),
                vmem((chips, share, channels), bf16), vmem((chips, share, channels), bf16),
                vmem((share, channels), bf16), vmem((2, chips, share, channels), bf16),
                vmem((replicas, per, LANES), f32), vmem((replicas, per, LANES), f32),
                vmem((per, LANES), f32), vmem((replicas, per, LANES), f32),
                dma((micros + 1,)), dma((micros,)), dma((micros,)),
                *[dma, dma((micros,))] * 7,
                dma, dma((micros,)), dma, dma, dma, dma, dma, dma((chips - 1,)), dma, dma, dma, dma, dma, dma,
            ],
            compiler_params=pltpu.CompilerParams(collective_id=0, has_side_effects=True),
        )(acts, out_grad, depth_kernel, point_weight, bn_gain)
        grads, point, kgrad, ggrad, bgrad = pl.pallas_call(
            finish,
            out_shape=(
                jax.ShapeDtypeStruct(acts.shape, bf16),
                jax.ShapeDtypeStruct((1, channels, channels), f32),
                jax.ShapeDtypeStruct((3, 3, 1, channels), f32),
                jax.ShapeDtypeStruct((1, channels), f32),
                jax.ShapeDtypeStruct((1, channels), f32),
            ),
            in_specs=[any_space, any_space, in_vmem, in_vmem, in_vmem],
            out_specs=(any_space, any_space, in_vmem, in_vmem, in_vmem),
            scratch_shapes=[
                vmem((micros, *acts.shape[2:]), bf16),
                vmem((channels, channels), bf16), vmem((channels, channels), f32),
                *[dma((micros,))] * 4,
            ],
        )(*results)
        return grads, point, jnp.transpose(kgrad, (2, 0, 1, 3)), ggrad, bgrad

    return jax.shard_map(
        body,
        mesh=mesh,
        in_specs=(
            P("section", None, "dp", None, None, None),
            P(None, "dp", None, None, None),
            P("section", None, None, None),
            P("section", None, None),
            P("section", None),
        ),
        out_specs=(
            P("section", None, "dp", None, None, None),
            P("section", None, None),
            P("section", None, None, None),
            P("section", None),
            P("section", None),
        ),
        check_vma=False,
    )
```

```python
import functools

import jax
import jax.numpy as jnp
from jax import lax
from jax.experimental import pallas as pl
from jax.experimental.pallas import tpu as pltpu
from jax.sharding import PartitionSpec as P

MESH = pl.DeviceIdType.MESH
epsilon = 1e-05
LANES = 128
BEFORE, FIRST = 1, 1


def columns_of(x, width):
    rows = x.shape[0]
    at = lax.broadcasted_iota(jnp.int32, x.shape, 0) % width
    before = jnp.where(at == 0, 0.0, pltpu.roll(x, 1, 0))
    after = jnp.where(at == width - 1, 0.0, pltpu.roll(x, rows - 1, 0))
    return before, x, after


def down(x, width):
    return jnp.concatenate([jnp.zeros((width, x.shape[1]), x.dtype), x[:-width]], axis=0)


def up(x, width):
    return jnp.concatenate([x[width:], jnp.zeros((width, x.shape[1]), x.dtype)], axis=0)


def ring(a, n):
    return min(a, n - a)


def offsets(ys, xs):
    every = [(y, x, 0) for y in range(ys) for x in range(xs)]
    return sorted(every, key=lambda o: -(ring(o[0], ys) + ring(o[1], xs)))


def kernel(
    ys, xs,
    sections, replicas, micros, height, width, channels,
    acts, out_grad, kern, weight, gain,
    out, point, kgrad, ggrad, bgrad,
    x_v, w_v, kf, depth, normed, nsend, nrecv, ubuf, usend, pgs, dgs,
    ones, lows, base, cmsg, crecv,
    mbuf, dmsg, dbuf, hmsg, hbuf, sums_of, smsg, obuf, omsg, tbuf, tmsg, stat, gacc,
    pacc, pair_src, pair_buf, rs_src, rs_buf, ag_src, ag_buf, kacc, krs_buf, kag_src, kag_buf,
    in_sem, og_sem, out_sem,
    t_send, t_recv, n_send, n_recv, c_send, c_recv, u_send, u_recv, x_send, x_recv, d_send, d_recv, o_send, o_recv,
    h_send, h_recv, w_send, w_recv, rs_send, rs_recv, ag_send, ag_recv, m_send, m_recv, ks_send, ks_recv, kg_send, kg_recv,
):
    f32, bf16 = jnp.float32, jnp.bfloat16
    sec = lax.axis_index("section")
    me = lax.axis_index("dp")
    rows = height * width
    chunks = channels // LANES
    count = replicas * rows
    last = sections - 1
    below = (sec + sections - 1) % sections
    above = (sec + 1) % sections

    def lanes(c):
        return slice(c * LANES, (c + 1) * LANES)

    for m in range(micros):
        pltpu.make_async_copy(acts.at[0, m, 0], x_v.at[m], in_sem.at[m]).start()
        if m == 0:
            pltpu.make_async_copy(weight.at[0], w_v, in_sem.at[micros]).start()

    @pl.when(sec == last)
    def _():
        for m in range(micros):
            pltpu.make_async_copy(out_grad.at[m, 0], ubuf.at[m], og_sem.at[m]).start()

    barrier = pltpu.get_barrier_semaphore()

    def greet(k, _):
        peer = (me + k) % replicas
        pl.semaphore_signal(barrier, inc=1, device_id={"section": below, "dp": peer}, device_id_type=MESH)
        pl.semaphore_signal(barrier, inc=1, device_id={"section": above, "dp": peer}, device_id_type=MESH)

        @pl.when(k > 0)
        def _():
            pl.semaphore_signal(barrier, inc=1, device_id={"section": sec, "dp": peer}, device_id_type=MESH)

        return 0

    lax.fori_loop(0, replicas, greet, 0)

    for i in range(3):
        for j in range(3):
            kf[3 * i + j] = jnp.reshape(kern[0, i, j].astype(f32), (1, channels))
    kacc[...] = jnp.zeros(kacc.shape, f32)
    gacc[...] = jnp.zeros(gacc.shape, f32)
    pacc[...] = jnp.zeros(pacc.shape, f32)

    def tap(i, j, c):
        return kf[3 * i + j, :, lanes(c)]

    def convolve(x, c):
        parts = columns_of(x, width)
        line = [sum(tap(i, j, c) * parts[j] for j in range(3)) for i in range(3)]
        return down(line[0], width) + line[1] + up(line[2], width)

    core, at_x, at_y = me % 2, (me // 2) % xs, me // (2 * xs)
    mate = me + 1 - 2 * core
    chips_from = offsets(ys, xs)

    def device_at(offset):
        dy, dx, dc = offset
        return (((at_y + dy) % ys) * xs + (at_x + dx) % xs) * 2 + (core + dc) % 2

    def to_peer(src, dst, send, recv, section, peer):
        pltpu.make_async_remote_copy(
            src_ref=src, dst_ref=dst, send_sem=send, recv_sem=recv,
            device_id={"section": section, "dp": peer}, device_id_type=MESH,
        ).start()

    def to_plane(section, src, dst, send, recv, first):
        def one(k, _):
            peer = (me + k) % replicas
            pltpu.make_async_remote_copy(
                src_ref=src(peer), dst_ref=dst, send_sem=send, recv_sem=recv,
                device_id={"section": section, "dp": peer}, device_id_type=MESH,
            ).start()
            return 0

        lax.fori_loop(first, replicas, one, 0)

    def wait_bytes(ref, sem):
        pltpu.make_async_copy(ref, ref, sem).wait()

    def row_sum(x):
        return jnp.sum(x, axis=0, keepdims=True)

    def forward(m, _):
        pltpu.make_async_copy(acts.at[0, m, 0], x_v.at[m], in_sem.at[m]).wait()
        for c in range(chunks):
            x = x_v[m, :, :, lanes(c)].astype(f32).reshape(rows, LANES)
            depth[m, :, lanes(c)] = convolve(jnp.maximum(x, 0.0), c).astype(bf16)

        @pl.when(m == 0)
        def _():
            pltpu.make_async_copy(weight.at[0], w_v, in_sem.at[micros]).wait()

        normed[m] = jnp.dot(depth[m], w_v[...], preferred_element_type=f32)
        for c in range(chunks):
            pre = normed[m, :, lanes(c)]
            tmsg[m, c : c + 1, :] = row_sum(pre)
            tmsg[m, chunks + c : chunks + c + 1, :] = row_sum(pre * pre)
            cmsg[m, c : c + 1, :] = tmsg[m, c : c + 1, :] / rows
            nsend[m, :, lanes(c)] = (pre - cmsg[m, c : c + 1, :]).astype(bf16)

        @pl.when(m == 0)
        def _():
            pl.semaphore_wait(barrier, 3 * replicas - 1)

        @pl.when(sec < last)
        def _():
            for src, dst, send, recv in ((cmsg, crecv, c_send, c_recv), (nsend, nrecv, n_send, n_recv)):
                pltpu.make_async_remote_copy(
                    src_ref=src.at[m], dst_ref=dst.at[m], send_sem=send, recv_sem=recv.at[m],
                    device_id={"section": above, "dp": me}, device_id_type=MESH,
                ).start()

        to_plane(sec, lambda _: tmsg.at[m], tbuf.at[m, me], t_send, t_recv.at[m], 1)
        tbuf[m, me] = tmsg[m]

        @pl.when(sec == last)
        def _():
            pltpu.make_async_copy(out_grad.at[m, 0], ubuf.at[m], og_sem.at[m]).wait()
            for c in range(chunks):
                u = ubuf[m, :, :, lanes(c)].astype(f32).reshape(rows, LANES)
                omsg[m, c : c + 1, :] = row_sum(u)
                omsg[m, chunks + c : chunks + c + 1, :] = row_sum(u * normed[m, :, lanes(c)])
            to_plane(sec, lambda _: omsg.at[m], obuf.at[m, me], o_send, o_recv.at[m], 1)
            obuf[m, me] = omsg[m]

        return 0

    lax.fori_loop(0, micros, forward, 0)

    def prepare(m):
        wait_bytes(tbuf.at[m, pl.ds(0, replicas - 1)], t_recv.at[m])
        total = jnp.sum(tbuf[m], axis=0) / count
        center = total[:chunks]
        inv_std = lax.rsqrt(total[chunks:] - center * center + epsilon)
        stat[0:chunks, :] = center
        stat[chunks:, :] = inv_std
        for c in range(chunks):
            normed[m, :, lanes(c)] = (normed[m, :, lanes(c)] - center[c : c + 1]) * inv_std[c : c + 1]

        @pl.when(sec > 0)
        def _():
            for c in range(chunks):
                x = x_v[m, :, :, lanes(c)].astype(f32).reshape(rows, LANES)
                ones[:, lanes(c)] = convolve(jnp.where(x > 0, 1.0, 0.0), c)
            wait_bytes(nrecv.at[m], n_recv.at[m])
            wait_bytes(crecv.at[m], c_recv.at[m])
            for c in range(chunks):
                x = x_v[m, :, :, lanes(c)].astype(f32).reshape(rows, LANES)
                low = nrecv[m, :, lanes(c)].astype(f32)
                lows[:, lanes(c)] = convolve(jnp.where(x > 0, low, 0.0), c)

    def critical(m):
        @pl.when(sec == last)
        def _():
            wait_bytes(obuf.at[m, pl.ds(0, replicas - 1)], o_recv.at[m])
            sums_of[...] = jnp.sum(obuf[m], axis=0).reshape(sums_of.shape)

        @pl.when(sec < last)
        def _():
            wait_bytes(dbuf.at[m], d_recv.at[m])
            hmsg[m] = jnp.sum(dbuf[m].astype(f32), axis=0)
            to_peer(hmsg.at[m], hbuf.at[m], h_send, h_recv.at[m], sec, mate)
            sums_of[core] = hmsg[m]
            wait_bytes(hbuf.at[m], h_recv.at[m])
            sums_of[1 - core] = hbuf[m]

        center, inv_std = stat[0:chunks, :], stat[chunks:, :]
        sum_grad = sums_of[0]
        cross = inv_std * (sums_of[1] - center * sum_grad)
        gacc[0:chunks, :] += sum_grad
        gacc[chunks:, :] += cross
        half = channels // 2
        for h in range(2):

            @pl.when(sec < last)
            def _():
                wait_bytes(ubuf.at[m, :, :, pl.ds(h * half, half)], u_recv.at[m, h])

            for c in range(h * chunks // 2, (h + 1) * chunks // 2):
                scale = gain[0:1, lanes(c)] * inv_std[c : c + 1]
                shift = scale * sum_grad[c : c + 1] / count
                slope = scale * cross[c : c + 1] / count
                u = ubuf[m, :, :, lanes(c)].astype(f32).reshape(rows, LANES)
                pgs[:, lanes(c)] = (scale * u - shift - slope * normed[m, :, lanes(c)]).astype(bf16)
                base[c : c + 1, :] = row_sum(u)
                base[chunks + c : chunks + c + 1, :] = row_sum(u * nrecv[m, :, lanes(c)].astype(f32))
            at = slice(h * half, (h + 1) * half)
            term = lax.dot_general(pgs[:, at], w_v[:, at], (((1,), (1,)), ((), ())), preferred_element_type=f32)
            dgs[...] = term if h == 0 else dgs[...] + term

        def send_on(c):
            to_peer(
                usend.at[m, :, :, pl.ds(c * LANES, LANES)], ubuf.at[m, :, :, pl.ds(c * LANES, LANES)],
                u_send, u_recv.at[m, c * 2 // chunks], below, me,
            )

        def gradient(c):
            parts = columns_of(dgs[:, lanes(c)], width)[::-1]
            line = [sum(tap(i, j, c) * parts[j] for j in range(3)) for i in range(3)]
            back = up(line[0], width) + line[1] + down(line[2], width)
            u = ubuf[m, :, :, lanes(c)].astype(f32).reshape(rows, LANES)
            x = x_v[m, :, :, lanes(c)].astype(f32).reshape(rows, LANES)
            result = (u + jnp.where(x > 0, back, 0.0)).astype(bf16)
            usend[m, :, :, lanes(c)] = result.reshape(height, width, LANES)

        for c in range(BEFORE):
            gradient(c)

        @pl.when(sec > 0)
        def _():
            for c in range(BEFORE):
                send_on(c)
            for c in range(chunks):
                grad = dgs[:, lanes(c)]
                plain = base[c : c + 1, :] + row_sum(grad * ones[:, lanes(c)])
                mixed = base[chunks + c : chunks + c + 1, :] + row_sum(grad * lows[:, lanes(c)])
                smsg[m, 0, c : c + 1, :] = plain
                smsg[m, 1, c : c + 1, :] = mixed + crecv[m, c : c + 1, :] * plain
            to_peer(smsg.at[m, 1 - core], mbuf.at[m], x_send, x_recv.at[m], sec, mate)

        for c in range(BEFORE, chunks):
            gradient(c)
            if c < FIRST:

                @pl.when(sec > 0)
                def _():
                    send_on(c)

        @pl.when(sec > 0)
        def _():
            wait_bytes(mbuf.at[m], x_recv.at[m])
            dmsg[m] = (smsg[m, core] + mbuf[m]).astype(bf16)
            for k, o in enumerate(chips_from):
                to_peer(dmsg.at[m], dbuf.at[m, k], d_send, d_recv.at[m], below, device_at(o))
            for c in range(FIRST, chunks):
                send_on(c)

        pltpu.make_async_copy(usend.at[m], out.at[0, m, 0], out_sem.at[m]).start()

    def weights(m):
        pacc[...] += lax.dot_general(
            depth[m], pgs[...], (((0,), (0,)), ((), ())), preferred_element_type=f32
        )
        per = kacc.shape[1]
        for c in range(chunks):
            x = x_v[m, :, :, lanes(c)].astype(f32).reshape(rows, LANES)
            active = jnp.maximum(x, 0.0)
            parts = columns_of(dgs[:, lanes(c)], width)[::-1]
            for i in range(3):
                for j in range(3):
                    moved = (up(parts[j], width), parts[j], down(parts[j], width))[i]
                    r = (3 * i + j) * chunks + c
                    kacc[r // per, r % per : r % per + 1, :] += row_sum(active * moved)

    def backward(m, _):
        critical(m)
        weights(m)

        @pl.when(m < micros - 1)
        def _():
            prepare(m + 1)
        return 0

    @pl.when(sec == 0)
    def _():
        nrecv[...] = jnp.zeros(nrecv.shape, bf16)

    prepare(0)
    lax.fori_loop(0, micros, backward, 0)

    per = kacc.shape[1]
    for k in range(2 * chunks):
        r = 9 * chunks + k
        kacc[r // per, r % per : r % per + 1, :] = jnp.where(me == 0, gacc[k : k + 1, :], 0.0)

    half = channels // 2
    chip = me // 2
    chips = replicas // 2
    others = chips_from[:-1]
    mine, its = pl.ds(pl.multiple_of(core * half, half), half), pl.ds(pl.multiple_of((1 - core) * half, half), half)
    pair_src[...] = pacc[its, :].astype(bf16)
    to_peer(pair_src, pair_buf, w_send, w_recv, sec, mate)
    to_plane(sec, lambda peer: kacc.at[peer], krs_buf.at[me], ks_send, ks_recv, 1)
    krs_buf[me] = kacc[me]
    wait_bytes(pair_buf, w_recv)
    rs_src[...] = (pacc[mine, :] + pair_buf[...].astype(f32)).astype(bf16).reshape(rs_src.shape)
    for o in others:
        peer = device_at(o)
        to_peer(rs_src.at[peer // 2], rs_buf.at[chip], rs_send, rs_recv, sec, peer)
    rs_buf[chip] = rs_src[chip]
    wait_bytes(krs_buf.at[pl.ds(0, replicas - 1)], ks_recv)
    kag_src[...] = jnp.sum(krs_buf[...], axis=0)
    wait_bytes(rs_buf.at[pl.ds(0, chips - 1)], rs_recv)
    ag_src[...] = jnp.sum(rs_buf[...].astype(f32), axis=0).astype(bf16)
    for k, o in enumerate(others):
        to_peer(ag_src, ag_buf.at[core, chip], ag_send, ag_recv.at[k], sec, device_at(o))
    to_peer(ag_src, ag_buf.at[core, chip], ag_send, m_recv, sec, mate)
    ag_buf[core, chip] = ag_src[...]
    to_plane(sec, lambda _: kag_src, kag_buf.at[me], kg_send, kg_recv, 1)
    kag_buf[me] = kag_src[...]
    for k, o in reversed(list(enumerate(others))):
        source = device_at((-o[0], -o[1], 0)) // 2
        wait_bytes(ag_src, ag_recv.at[k])
        to_peer(ag_buf.at[core, source], ag_buf.at[core, source], m_send, m_recv, sec, mate)
    wait_bytes(kag_buf.at[pl.ds(0, replicas - 1)], kg_recv)
    for t in range(9):
        for c in range(chunks):
            r = t * chunks + c
            kgrad[0, t // 3, t % 3 : t % 3 + 1, lanes(c)] = kag_buf[r // per, r % per : r % per + 1, :]
    for c in range(chunks):
        for at, ref in ((9, bgrad), (10, ggrad)):
            r = at * chunks + c
            ref[0:1, lanes(c)] = kag_buf[r // per, r % per : r % per + 1, :]
    wait_bytes(ag_buf.at[0], m_recv)
    point[0] = ag_buf[...].reshape(channels, channels)

    for m in range(micros):
        pltpu.make_async_copy(usend.at[m], out.at[0, m, 0], out_sem.at[m]).wait()
    wait_bytes(tbuf.at[:, pl.ds(0, replicas - 1)], t_send)

    @pl.when(sec < last)
    def _():
        wait_bytes(nsend, n_send)
        wait_bytes(hbuf, h_send)
        wait_bytes(cmsg, c_send)

    @pl.when(sec == last)
    def _():
        wait_bytes(obuf.at[:, pl.ds(0, replicas - 1)], o_send)

    @pl.when(sec > 0)
    def _():
        wait_bytes(usend, u_send)
        wait_bytes(mbuf, x_send)
        wait_bytes(dbuf, d_send)

    wait_bytes(pair_src, w_send)
    wait_bytes(rs_buf.at[pl.ds(0, chips - 1)], rs_send)
    wait_bytes(rs_buf.at[pl.ds(0, chips - 1)], m_send)
    wait_bytes(krs_buf.at[pl.ds(0, replicas - 1)], ks_send)
    wait_bytes(rs_buf, ag_send)
    wait_bytes(kag_buf.at[pl.ds(0, replicas - 1)], kg_send)


def finish(grads, point, kgrad, ggrad, bgrad, grads_out, point_out, kgrad_out, ggrad_out, bgrad_out, held, narrow, wide, in_sem, out_sem, p_in, p_out):
    parts = grads.shape[1]
    share = point.shape[1] // parts

    def point_copy(m, back):
        at = pl.ds(m * share, share)
        if back:
            return pltpu.make_async_copy(wide.at[at], point_out.at[0, at], p_out.at[m])
        return pltpu.make_async_copy(point.at[0, at], narrow.at[at], p_in.at[m])

    def grads_copy(m, back):
        if back:
            return pltpu.make_async_copy(held.at[m], grads_out.at[0, m], out_sem.at[m])
        return pltpu.make_async_copy(grads.at[0, m], held.at[m], in_sem.at[m])

    for m in range(parts):
        point_copy(m, False).start()
        grads_copy(m, False).start()
    for t in range(9):
        kgrad_out[t // 3, t % 3, 0:1, :] = kgrad[0, t // 3, t % 3 : t % 3 + 1, :]
    ggrad_out[...] = ggrad[...]
    bgrad_out[...] = bgrad[...]
    for m in range(parts):
        at = slice(m * share, (m + 1) * share)
        point_copy(m, False).wait()
        wide[at, :] = narrow[at, :].astype(jnp.float32)
        point_copy(m, True).start()
        grads_copy(m, False).wait()
        grads_copy(m, True).start()
    for m in range(parts):
        point_copy(m, True).wait()
        grads_copy(m, True).wait()


def solution(mesh):
    sections, replicas = mesh.shape["section"], mesh.shape["dp"]
    chips = replicas // 2
    ys = max(y for y in range(1, chips + 1) if y * y <= chips and chips % y == 0)
    xs = chips // ys

    def body(acts, out_grad, depth_kernel, point_weight, bn_gain):
        micros, _, height, width, channels = acts.shape[1:]
        rows = height * width
        chunks = channels // LANES
        share = channels // replicas
        per = -(-11 * chunks // replicas)
        f32, bf16 = jnp.float32, jnp.bfloat16
        image = (micros, height, width, channels)
        flat = (micros, rows, channels)
        sums, kind = (2 * chunks, LANES), (chunks, LANES)
        vmem, dma = pltpu.VMEM, pltpu.SemaphoreType.DMA
        any_space = pl.BlockSpec(memory_space=pl.ANY)
        in_vmem = pl.BlockSpec(memory_space=pltpu.VMEM)
        results = pl.pallas_call(
            functools.partial(kernel, ys, xs, sections, replicas, micros, height, width, channels),
            out_shape=(
                jax.ShapeDtypeStruct(acts.shape, bf16),
                jax.ShapeDtypeStruct((1, channels, channels), bf16),
                jax.ShapeDtypeStruct((1, 3, 3, channels), f32),
                jax.ShapeDtypeStruct((1, channels), f32),
                jax.ShapeDtypeStruct((1, channels), f32),
            ),
            in_specs=[any_space, any_space, in_vmem, any_space, in_vmem],
            out_specs=(any_space, in_vmem, in_vmem, in_vmem, in_vmem),
            scratch_shapes=[
                vmem(image, bf16), vmem((channels, channels), bf16), vmem((9, 1, channels), f32),
                vmem(flat, bf16), vmem(flat, f32), vmem(flat, bf16), vmem(flat, bf16),
                vmem(image, bf16), vmem(image, bf16), vmem((rows, channels), bf16), vmem((rows, channels), f32),
                vmem((rows, channels), f32), vmem((rows, channels), f32), vmem(sums, f32),
                vmem((micros, chunks, LANES), f32), vmem((micros, chunks, LANES), f32),
                vmem((micros, *kind), f32), vmem((micros, *kind), bf16), vmem((micros, chips, *kind), bf16),
                vmem((micros, *kind), f32), vmem((micros, *kind), f32), vmem((2, *kind), f32), vmem((micros, 2, *kind), f32),
                vmem((micros, replicas, *sums), f32), vmem((micros, *sums), f32),
                vmem((micros, replicas, *sums), f32), vmem((micros, *sums), f32),
                vmem(sums, f32), vmem(sums, f32),
                vmem((channels, channels), f32),
                vmem((channels // 2, channels), bf16), vmem((channels // 2, channels), bf16),
                vmem((chips, share, channels), bf16), vmem((chips, share, channels), bf16),
                vmem((share, channels), bf16), vmem((2, chips, share, channels), bf16),
                vmem((replicas, per, LANES), f32), vmem((replicas, per, LANES), f32),
                vmem((per, LANES), f32), vmem((replicas, per, LANES), f32),
                dma((micros + 1,)), dma((micros,)), dma((micros,)),
                *[dma, dma((micros,))] * 3, dma, dma((micros, 2)), *[dma, dma((micros,))] * 3,
                dma, dma((micros,)), dma, dma, dma, dma, dma, dma((chips - 1,)), dma, dma, dma, dma, dma, dma,
            ],
            compiler_params=pltpu.CompilerParams(collective_id=0, has_side_effects=True),
        )(acts, out_grad, depth_kernel, point_weight, bn_gain)
        grads, point, kgrad, ggrad, bgrad = pl.pallas_call(
            finish,
            out_shape=(
                jax.ShapeDtypeStruct(acts.shape, bf16),
                jax.ShapeDtypeStruct((1, channels, channels), f32),
                jax.ShapeDtypeStruct((3, 3, 1, channels), f32),
                jax.ShapeDtypeStruct((1, channels), f32),
                jax.ShapeDtypeStruct((1, channels), f32),
            ),
            in_specs=[any_space, any_space, in_vmem, in_vmem, in_vmem],
            out_specs=(any_space, any_space, in_vmem, in_vmem, in_vmem),
            scratch_shapes=[
                vmem((micros, *acts.shape[2:]), bf16),
                vmem((channels, channels), bf16), vmem((channels, channels), f32),
                *[dma((micros,))] * 4,
            ],
        )(*results)
        return grads, point, jnp.transpose(kgrad, (2, 0, 1, 3)), ggrad, bgrad

    return jax.shard_map(
        body,
        mesh=mesh,
        in_specs=(
            P("section", None, "dp", None, None, None),
            P(None, "dp", None, None, None),
            P("section", None, None, None),
            P("section", None, None),
            P("section", None),
        ),
        out_specs=(
            P("section", None, "dp", None, None, None),
            P("section", None, None),
            P("section", None, None, None),
            P("section", None),
            P("section", None),
        ),
        check_vma=False,
    )
```

```python
import functools

import jax
import jax.numpy as jnp
from jax import lax
from jax.experimental import pallas as pl
from jax.experimental.pallas import tpu as pltpu
from jax.sharding import PartitionSpec as P

MESH = pl.DeviceIdType.MESH
epsilon = 1e-05
LANES = 128
BEFORE, FIRST = 1, 1


def columns_of(x, width):
    rows = x.shape[0]
    at = lax.broadcasted_iota(jnp.int32, x.shape, 0) % width
    before = jnp.where(at == 0, 0.0, pltpu.roll(x, 1, 0))
    after = jnp.where(at == width - 1, 0.0, pltpu.roll(x, rows - 1, 0))
    return before, x, after


def down(x, width):
    return jnp.concatenate([jnp.zeros((width, x.shape[1]), x.dtype), x[:-width]], axis=0)


def up(x, width):
    return jnp.concatenate([x[width:], jnp.zeros((width, x.shape[1]), x.dtype)], axis=0)


def ring(a, n):
    return min(a, n - a)


def offsets(ys, xs):
    every = [(y, x, 0) for y in range(ys) for x in range(xs)]
    return sorted(every, key=lambda o: -(ring(o[0], ys) + ring(o[1], xs)))


def kernel(
    ys, xs,
    sections, replicas, micros, height, width, channels,
    acts, out_grad, kern_in, weight, gain_in,
    out, point, kgrad, ggrad, bgrad,
    kern, gain, x_v, w_v, kf, depth, normed, nsend, nrecv, ubuf, usend, pgs, dgs,
    ones, lows, base, cmsg, crecv,
    mbuf, dmsg, dbuf, hmsg, hbuf, sums_of, smsg, obuf, omsg, tbuf, tmsg, stat, gacc,
    pacc, pair_src, pair_buf, rs_src, rs_buf, ag_src, ag_buf, kacc, krs_buf, kag_src, kag_buf,
    in_sem, og_sem, out_sem,
    t_send, t_recv, n_send, n_recv, c_send, c_recv, u_send, u_recv, x_send, x_recv, d_send, d_recv, o_send, o_recv,
    h_send, h_recv, w_send, w_recv, rs_send, rs_recv, ag_send, ag_recv, m_send, m_recv, ks_send, ks_recv, kg_send, kg_recv,
):
    f32, bf16 = jnp.float32, jnp.bfloat16
    sec = lax.axis_index("section")
    me = lax.axis_index("dp")
    rows = height * width
    chunks = channels // LANES
    count = replicas * rows
    last = sections - 1
    below = (sec + sections - 1) % sections
    above = (sec + 1) % sections

    def lanes(c):
        return slice(c * LANES, (c + 1) * LANES)

    small = ((kern_in, kern, micros + 1), (gain_in, gain, micros + 2))
    for src, dst, k in small:
        pltpu.make_async_copy(src, dst, in_sem.at[k]).start()
    for m in range(micros):
        pltpu.make_async_copy(acts.at[0, m, 0], x_v.at[m], in_sem.at[m]).start()
        if m == 0:
            pltpu.make_async_copy(weight.at[0], w_v, in_sem.at[micros]).start()

    @pl.when(sec == last)
    def _():
        for m in range(micros):
            pltpu.make_async_copy(out_grad.at[m, 0], ubuf.at[m], og_sem.at[m]).start()

    barrier = pltpu.get_barrier_semaphore()

    def greet(k, _):
        peer = (me + k) % replicas
        pl.semaphore_signal(barrier, inc=1, device_id={"section": below, "dp": peer}, device_id_type=MESH)
        pl.semaphore_signal(barrier, inc=1, device_id={"section": above, "dp": peer}, device_id_type=MESH)

        @pl.when(k > 0)
        def _():
            pl.semaphore_signal(barrier, inc=1, device_id={"section": sec, "dp": peer}, device_id_type=MESH)

        return 0

    lax.fori_loop(0, replicas, greet, 0)

    for src, dst, k in small:
        pltpu.make_async_copy(src, dst, in_sem.at[k]).wait()
    for i in range(3):
        for j in range(3):
            kf[3 * i + j] = jnp.reshape(kern[0, i, j].astype(f32), (1, channels))
    kacc[...] = jnp.zeros(kacc.shape, f32)
    gacc[...] = jnp.zeros(gacc.shape, f32)
    pacc[...] = jnp.zeros(pacc.shape, f32)

    def tap(i, j, c):
        return kf[3 * i + j, :, lanes(c)]

    def convolve(x, c):
        parts = columns_of(x, width)
        line = [sum(tap(i, j, c) * parts[j] for j in range(3)) for i in range(3)]
        return down(line[0], width) + line[1] + up(line[2], width)

    core, at_x, at_y = me % 2, (me // 2) % xs, me // (2 * xs)
    mate = me + 1 - 2 * core
    chips_from = offsets(ys, xs)

    def device_at(offset):
        dy, dx, dc = offset
        return (((at_y + dy) % ys) * xs + (at_x + dx) % xs) * 2 + (core + dc) % 2

    def to_peer(src, dst, send, recv, section, peer):
        pltpu.make_async_remote_copy(
            src_ref=src, dst_ref=dst, send_sem=send, recv_sem=recv,
            device_id={"section": section, "dp": peer}, device_id_type=MESH,
        ).start()

    def to_plane(section, src, dst, send, recv, first):
        def one(k, _):
            peer = (me + k) % replicas
            pltpu.make_async_remote_copy(
                src_ref=src(peer), dst_ref=dst, send_sem=send, recv_sem=recv,
                device_id={"section": section, "dp": peer}, device_id_type=MESH,
            ).start()
            return 0

        lax.fori_loop(first, replicas, one, 0)

    def wait_bytes(ref, sem):
        pltpu.make_async_copy(ref, ref, sem).wait()

    def row_sum(x):
        return jnp.sum(x, axis=0, keepdims=True)

    def forward(m, _):
        pltpu.make_async_copy(acts.at[0, m, 0], x_v.at[m], in_sem.at[m]).wait()
        for c in range(chunks):
            x = x_v[m, :, :, lanes(c)].astype(f32).reshape(rows, LANES)
            depth[m, :, lanes(c)] = convolve(jnp.maximum(x, 0.0), c).astype(bf16)

        @pl.when(m == 0)
        def _():
            pltpu.make_async_copy(weight.at[0], w_v, in_sem.at[micros]).wait()

        normed[m] = jnp.dot(depth[m], w_v[...], preferred_element_type=f32)
        for c in range(chunks):
            pre = normed[m, :, lanes(c)]
            tmsg[m, c : c + 1, :] = row_sum(pre)
            tmsg[m, chunks + c : chunks + c + 1, :] = row_sum(pre * pre)
            cmsg[m, c : c + 1, :] = tmsg[m, c : c + 1, :] / rows
            nsend[m, :, lanes(c)] = (pre - cmsg[m, c : c + 1, :]).astype(bf16)

        @pl.when(m == 0)
        def _():
            pl.semaphore_wait(barrier, 3 * replicas - 1)

        @pl.when(sec < last)
        def _():
            for src, dst, send, recv in ((cmsg, crecv, c_send, c_recv), (nsend, nrecv, n_send, n_recv)):
                pltpu.make_async_remote_copy(
                    src_ref=src.at[m], dst_ref=dst.at[m], send_sem=send, recv_sem=recv.at[m],
                    device_id={"section": above, "dp": me}, device_id_type=MESH,
                ).start()

        to_plane(sec, lambda _: tmsg.at[m], tbuf.at[m, me], t_send, t_recv.at[m], 1)
        tbuf[m, me] = tmsg[m]

        @pl.when(sec == last)
        def _():
            pltpu.make_async_copy(out_grad.at[m, 0], ubuf.at[m], og_sem.at[m]).wait()
            for c in range(chunks):
                u = ubuf[m, :, :, lanes(c)].astype(f32).reshape(rows, LANES)
                omsg[m, c : c + 1, :] = row_sum(u)
                omsg[m, chunks + c : chunks + c + 1, :] = row_sum(u * normed[m, :, lanes(c)])
            to_plane(sec, lambda _: omsg.at[m], obuf.at[m, me], o_send, o_recv.at[m], 1)
            obuf[m, me] = omsg[m]

        return 0

    lax.fori_loop(0, micros, forward, 0)

    def prepare(m):
        wait_bytes(tbuf.at[m, pl.ds(0, replicas - 1)], t_recv.at[m])
        total = jnp.sum(tbuf[m], axis=0) / count
        center = total[:chunks]
        inv_std = lax.rsqrt(total[chunks:] - center * center + epsilon)
        stat[0:chunks, :] = center
        stat[chunks:, :] = inv_std
        for c in range(chunks):
            normed[m, :, lanes(c)] = (normed[m, :, lanes(c)] - center[c : c + 1]) * inv_std[c : c + 1]

        @pl.when(sec > 0)
        def _():
            for c in range(chunks):
                x = x_v[m, :, :, lanes(c)].astype(f32).reshape(rows, LANES)
                ones[:, lanes(c)] = convolve(jnp.where(x > 0, 1.0, 0.0), c)
            wait_bytes(nrecv.at[m], n_recv.at[m])
            wait_bytes(crecv.at[m], c_recv.at[m])
            for c in range(chunks):
                x = x_v[m, :, :, lanes(c)].astype(f32).reshape(rows, LANES)
                low = nrecv[m, :, lanes(c)].astype(f32)
                lows[:, lanes(c)] = convolve(jnp.where(x > 0, low, 0.0), c)

    def critical(m):
        @pl.when(sec == last)
        def _():
            wait_bytes(obuf.at[m, pl.ds(0, replicas - 1)], o_recv.at[m])
            sums_of[...] = jnp.sum(obuf[m], axis=0).reshape(sums_of.shape)

        @pl.when(sec < last)
        def _():
            wait_bytes(dbuf.at[m], d_recv.at[m])
            hmsg[m] = jnp.sum(dbuf[m].astype(f32), axis=0)
            to_peer(hmsg.at[m], hbuf.at[m], h_send, h_recv.at[m], sec, mate)
            sums_of[core] = hmsg[m]
            wait_bytes(hbuf.at[m], h_recv.at[m])
            sums_of[1 - core] = hbuf[m]

        center, inv_std = stat[0:chunks, :], stat[chunks:, :]
        sum_grad = sums_of[0]
        cross = inv_std * (sums_of[1] - center * sum_grad)
        gacc[0:chunks, :] += sum_grad
        gacc[chunks:, :] += cross
        half = channels // 2
        for h in range(2):

            @pl.when(sec < last)
            def _():
                wait_bytes(ubuf.at[m, :, :, pl.ds(h * half, half)], u_recv.at[m, h])

            for c in range(h * chunks // 2, (h + 1) * chunks // 2):
                scale = gain[0:1, lanes(c)] * inv_std[c : c + 1]
                shift = scale * sum_grad[c : c + 1] / count
                slope = scale * cross[c : c + 1] / count
                u = ubuf[m, :, :, lanes(c)].astype(f32).reshape(rows, LANES)
                pgs[:, lanes(c)] = (scale * u - shift - slope * normed[m, :, lanes(c)]).astype(bf16)
                base[c : c + 1, :] = row_sum(u)
                base[chunks + c : chunks + c + 1, :] = row_sum(u * nrecv[m, :, lanes(c)].astype(f32))
            at = slice(h * half, (h + 1) * half)
            term = lax.dot_general(pgs[:, at], w_v[:, at], (((1,), (1,)), ((), ())), preferred_element_type=f32)
            dgs[...] = term if h == 0 else dgs[...] + term

        def send_on(c):
            to_peer(
                usend.at[m, :, :, pl.ds(c * LANES, LANES)], ubuf.at[m, :, :, pl.ds(c * LANES, LANES)],
                u_send, u_recv.at[m, c * 2 // chunks], below, me,
            )

        def gradient(c):
            parts = columns_of(dgs[:, lanes(c)], width)[::-1]
            line = [sum(tap(i, j, c) * parts[j] for j in range(3)) for i in range(3)]
            back = up(line[0], width) + line[1] + down(line[2], width)
            u = ubuf[m, :, :, lanes(c)].astype(f32).reshape(rows, LANES)
            x = x_v[m, :, :, lanes(c)].astype(f32).reshape(rows, LANES)
            result = (u + jnp.where(x > 0, back, 0.0)).astype(bf16)
            usend[m, :, :, lanes(c)] = result.reshape(height, width, LANES)

        for c in range(BEFORE):
            gradient(c)

        @pl.when(sec > 0)
        def _():
            for c in range(BEFORE):
                send_on(c)
            for c in range(chunks):
                grad = dgs[:, lanes(c)]
                plain = base[c : c + 1, :] + row_sum(grad * ones[:, lanes(c)])
                mixed = base[chunks + c : chunks + c + 1, :] + row_sum(grad * lows[:, lanes(c)])
                smsg[m, 0, c : c + 1, :] = plain
                smsg[m, 1, c : c + 1, :] = mixed + crecv[m, c : c + 1, :] * plain
            to_peer(smsg.at[m, 1 - core], mbuf.at[m], x_send, x_recv.at[m], sec, mate)

        for c in range(BEFORE, chunks):
            gradient(c)
            if c < FIRST:

                @pl.when(sec > 0)
                def _():
                    send_on(c)

        @pl.when(sec > 0)
        def _():
            wait_bytes(mbuf.at[m], x_recv.at[m])
            dmsg[m] = (smsg[m, core] + mbuf[m]).astype(bf16)
            for k, o in enumerate(chips_from):
                to_peer(dmsg.at[m], dbuf.at[m, k], d_send, d_recv.at[m], below, device_at(o))
            for c in range(FIRST, chunks):
                send_on(c)

        pltpu.make_async_copy(usend.at[m], out.at[0, m, 0], out_sem.at[m]).start()

    def weights(m):
        pacc[...] += lax.dot_general(
            depth[m], pgs[...], (((0,), (0,)), ((), ())), preferred_element_type=f32
        )

    def taps(m):
        per = kacc.shape[1]
        for c in range(chunks):
            x = x_v[m, :, :, lanes(c)].astype(f32).reshape(rows, LANES)
            active = jnp.maximum(x, 0.0)
            parts = columns_of(dgs[:, lanes(c)], width)[::-1]
            for i in range(3):
                for j in range(3):
                    moved = (up(parts[j], width), parts[j], down(parts[j], width))[i]
                    r = (3 * i + j) * chunks + c
                    kacc[r // per, r % per : r % per + 1, :] += row_sum(active * moved)

    def backward(m, _):
        critical(m)
        weights(m)

        @pl.when(m < micros - 1)
        def _():
            taps(m)
            prepare(m + 1)
        return 0

    @pl.when(sec == 0)
    def _():
        nrecv[...] = jnp.zeros(nrecv.shape, bf16)

    prepare(0)
    lax.fori_loop(0, micros, backward, 0)

    half = channels // 2
    chip = me // 2
    chips = replicas // 2
    others = chips_from[:-1]
    mine, its = pl.ds(pl.multiple_of(core * half, half), half), pl.ds(pl.multiple_of((1 - core) * half, half), half)
    pair_src[...] = pacc[its, :].astype(bf16)
    to_peer(pair_src, pair_buf, w_send, w_recv, sec, mate)
    taps(micros - 1)

    per = kacc.shape[1]
    for k in range(2 * chunks):
        r = 9 * chunks + k
        kacc[r // per, r % per : r % per + 1, :] = jnp.where(me == 0, gacc[k : k + 1, :], 0.0)

    to_plane(sec, lambda peer: kacc.at[peer], krs_buf.at[me], ks_send, ks_recv, 1)
    krs_buf[me] = kacc[me]
    wait_bytes(pair_buf, w_recv)
    rs_src[...] = (pacc[mine, :] + pair_buf[...].astype(f32)).astype(bf16).reshape(rs_src.shape)
    for o in others:
        peer = device_at(o)
        to_peer(rs_src.at[peer // 2], rs_buf.at[chip], rs_send, rs_recv, sec, peer)
    rs_buf[chip] = rs_src[chip]
    wait_bytes(krs_buf.at[pl.ds(0, replicas - 1)], ks_recv)
    kag_src[...] = jnp.sum(krs_buf[...], axis=0)
    wait_bytes(rs_buf.at[pl.ds(0, chips - 1)], rs_recv)
    ag_src[...] = jnp.sum(rs_buf[...].astype(f32), axis=0).astype(bf16)
    for k, o in enumerate(others):
        to_peer(ag_src, ag_buf.at[core, chip], ag_send, ag_recv.at[k], sec, device_at(o))
    to_peer(ag_src, ag_buf.at[core, chip], ag_send, m_recv, sec, mate)
    ag_buf[core, chip] = ag_src[...]
    to_plane(sec, lambda _: kag_src, kag_buf.at[me], kg_send, kg_recv, 1)
    kag_buf[me] = kag_src[...]
    for k, o in reversed(list(enumerate(others))):
        source = device_at((-o[0], -o[1], 0)) // 2
        wait_bytes(ag_src, ag_recv.at[k])
        to_peer(ag_buf.at[core, source], ag_buf.at[core, source], m_send, m_recv, sec, mate)
    wait_bytes(kag_buf.at[pl.ds(0, replicas - 1)], kg_recv)
    for t in range(9):
        for c in range(chunks):
            r = t * chunks + c
            kgrad[0, t // 3, t % 3 : t % 3 + 1, lanes(c)] = kag_buf[r // per, r % per : r % per + 1, :]
    for c in range(chunks):
        for at, ref in ((9, bgrad), (10, ggrad)):
            r = at * chunks + c
            ref[0:1, lanes(c)] = kag_buf[r // per, r % per : r % per + 1, :]
    wait_bytes(ag_buf.at[0], m_recv)
    point[0] = ag_buf[...].reshape(channels, channels)

    for m in range(micros):
        pltpu.make_async_copy(usend.at[m], out.at[0, m, 0], out_sem.at[m]).wait()
    wait_bytes(tbuf.at[:, pl.ds(0, replicas - 1)], t_send)

    @pl.when(sec < last)
    def _():
        wait_bytes(nsend, n_send)
        wait_bytes(hbuf, h_send)
        wait_bytes(cmsg, c_send)

    @pl.when(sec == last)
    def _():
        wait_bytes(obuf.at[:, pl.ds(0, replicas - 1)], o_send)

    @pl.when(sec > 0)
    def _():
        wait_bytes(usend, u_send)
        wait_bytes(mbuf, x_send)
        wait_bytes(dbuf, d_send)

    wait_bytes(pair_src, w_send)
    wait_bytes(rs_buf.at[pl.ds(0, chips - 1)], rs_send)
    wait_bytes(rs_buf.at[pl.ds(0, chips - 1)], m_send)
    wait_bytes(krs_buf.at[pl.ds(0, replicas - 1)], ks_send)
    wait_bytes(rs_buf, ag_send)
    wait_bytes(kag_buf.at[pl.ds(0, replicas - 1)], kg_send)


def finish(
    grads, point, kgrad, ggrad, bgrad, grads_out, point_out, kgrad_out, ggrad_out, bgrad_out,
    held, narrow, wide, k_in, k_out, g_held, b_held, in_sem, out_sem, p_in, p_out, s_in, s_out,
):
    parts = grads.shape[1]
    share = point.shape[1] // parts

    def point_copy(m, back):
        at = pl.ds(m * share, share)
        if back:
            return pltpu.make_async_copy(wide.at[at], point_out.at[0, at], p_out.at[m])
        return pltpu.make_async_copy(point.at[0, at], narrow.at[at], p_in.at[m])

    def grads_copy(m, back):
        if back:
            return pltpu.make_async_copy(held.at[m], grads_out.at[0, m], out_sem.at[m])
        return pltpu.make_async_copy(grads.at[0, m], held.at[m], in_sem.at[m])

    for m in range(parts):
        point_copy(m, False).start()
        grads_copy(m, False).start()
    ins = [pltpu.make_async_copy(a, b, s_in.at[k]) for k, (a, b) in enumerate(((kgrad, k_in), (ggrad, g_held), (bgrad, b_held)))]
    outs = [pltpu.make_async_copy(a, b, s_out.at[k]) for k, (a, b) in enumerate(((k_out, kgrad_out), (g_held, ggrad_out), (b_held, bgrad_out)))]
    for copy in ins:
        copy.start()
    for m in range(parts):
        at = slice(m * share, (m + 1) * share)
        point_copy(m, False).wait()
        wide[at, :] = narrow[at, :].astype(jnp.float32)
        point_copy(m, True).start()
        grads_copy(m, False).wait()
        grads_copy(m, True).start()
    for copy in ins:
        copy.wait()
    for t in range(9):
        k_out[t // 3, t % 3, 0:1, :] = k_in[0, t // 3, t % 3 : t % 3 + 1, :]
    for copy in outs:
        copy.start()
    for copy in outs:
        copy.wait()
    for m in range(parts):
        point_copy(m, True).wait()
        grads_copy(m, True).wait()


def solution(mesh):
    sections, replicas = mesh.shape["section"], mesh.shape["dp"]
    chips = replicas // 2
    ys = max(y for y in range(1, chips + 1) if y * y <= chips and chips % y == 0)
    xs = chips // ys

    def body(acts, out_grad, depth_kernel, point_weight, bn_gain):
        micros, _, height, width, channels = acts.shape[1:]
        rows = height * width
        chunks = channels // LANES
        share = channels // replicas
        per = -(-11 * chunks // replicas)
        f32, bf16 = jnp.float32, jnp.bfloat16
        image = (micros, height, width, channels)
        flat = (micros, rows, channels)
        sums, kind = (2 * chunks, LANES), (chunks, LANES)
        vmem, dma = pltpu.VMEM, pltpu.SemaphoreType.DMA
        any_space = pl.BlockSpec(memory_space=pl.ANY)
        in_vmem = pl.BlockSpec(memory_space=pltpu.VMEM)
        results = pl.pallas_call(
            functools.partial(kernel, ys, xs, sections, replicas, micros, height, width, channels),
            out_shape=(
                jax.ShapeDtypeStruct(acts.shape, bf16),
                jax.ShapeDtypeStruct((1, channels, channels), bf16),
                jax.ShapeDtypeStruct((1, 3, 3, channels), f32),
                jax.ShapeDtypeStruct((1, channels), f32),
                jax.ShapeDtypeStruct((1, channels), f32),
            ),
            in_specs=[any_space] * 5,
            out_specs=(any_space, in_vmem, in_vmem, in_vmem, in_vmem),
            scratch_shapes=[
                vmem((1, 3, 3, channels), bf16), vmem((1, channels), f32),
                vmem(image, bf16), vmem((channels, channels), bf16), vmem((9, 1, channels), f32),
                vmem(flat, bf16), vmem(flat, f32), vmem(flat, bf16), vmem(flat, bf16),
                vmem(image, bf16), vmem(image, bf16), vmem((rows, channels), bf16), vmem((rows, channels), f32),
                vmem((rows, channels), f32), vmem((rows, channels), f32), vmem(sums, f32),
                vmem((micros, chunks, LANES), f32), vmem((micros, chunks, LANES), f32),
                vmem((micros, *kind), f32), vmem((micros, *kind), bf16), vmem((micros, chips, *kind), bf16),
                vmem((micros, *kind), f32), vmem((micros, *kind), f32), vmem((2, *kind), f32), vmem((micros, 2, *kind), f32),
                vmem((micros, replicas, *sums), f32), vmem((micros, *sums), f32),
                vmem((micros, replicas, *sums), f32), vmem((micros, *sums), f32),
                vmem(sums, f32), vmem(sums, f32),
                vmem((channels, channels), f32),
                vmem((channels // 2, channels), bf16), vmem((channels // 2, channels), bf16),
                vmem((chips, share, channels), bf16), vmem((chips, share, channels), bf16),
                vmem((share, channels), bf16), vmem((2, chips, share, channels), bf16),
                vmem((replicas, per, LANES), f32), vmem((replicas, per, LANES), f32),
                vmem((per, LANES), f32), vmem((replicas, per, LANES), f32),
                dma((micros + 3,)), dma((micros,)), dma((micros,)),
                *[dma, dma((micros,))] * 3, dma, dma((micros, 2)), *[dma, dma((micros,))] * 3,
                dma, dma((micros,)), dma, dma, dma, dma, dma, dma((chips - 1,)), dma, dma, dma, dma, dma, dma,
            ],
            compiler_params=pltpu.CompilerParams(collective_id=0, has_side_effects=True),
        )(acts, out_grad, depth_kernel, point_weight, bn_gain)
        grads, point, kgrad, ggrad, bgrad = pl.pallas_call(
            finish,
            out_shape=(
                jax.ShapeDtypeStruct(acts.shape, bf16),
                jax.ShapeDtypeStruct((1, channels, channels), f32),
                jax.ShapeDtypeStruct((3, 3, 1, channels), f32),
                jax.ShapeDtypeStruct((1, channels), f32),
                jax.ShapeDtypeStruct((1, channels), f32),
            ),
            in_specs=[any_space] * 5,
            out_specs=(any_space,) * 5,
            scratch_shapes=[
                vmem((micros, *acts.shape[2:]), bf16),
                vmem((channels, channels), bf16), vmem((channels, channels), f32),
                vmem((1, 3, 3, channels), f32), vmem((3, 3, 1, channels), f32),
                vmem((1, channels), f32), vmem((1, channels), f32),
                *[dma((micros,))] * 4, dma((3,)), dma((3,)),
            ],
        )(*results)
        return grads, point, jnp.transpose(kgrad, (2, 0, 1, 3)), ggrad, bgrad

    return jax.shard_map(
        body,
        mesh=mesh,
        in_specs=(
            P("section", None, "dp", None, None, None),
            P(None, "dp", None, None, None),
            P("section", None, None, None),
            P("section", None, None),
            P("section", None),
        ),
        out_specs=(
            P("section", None, "dp", None, None, None),
            P("section", None, None),
            P("section", None, None, None),
            P("section", None),
            P("section", None),
        ),
        check_vma=False,
    )
```
